128 devices in a mesh: tensor: 4 (over z_hi, core), dp: 32 (over y, x, z_lo).
Axes of the slice: x: 4, y: 4, z: 4 (z_hi: 2, z_lo: 2; z = z_hi * 2 + z_lo), core: 2. Of those that a mesh axis runs over, the one named last changes fastest.
Arguments:
- grads: bfloat16 [32, 4, 8192, 1024], P('dp', None, None, 'tensor'), may hold values from -6 to 6
- param: float32 [4, 8192, 1024], P(None, 'dp', 'tensor'), may hold values from -3 to 3
- q_m: bfloat16 [4, 8192, 1024], P(None, 'dp', 'tensor'), may hold values from -1 to 1
- m_scale: float32 [4], replicated, may hold values from 0.02 to 0.2
- q_v: bfloat16 [4, 8192, 1024], P(None, 'dp', 'tensor'), may hold values from 0.0009994507 to 1
- v_max: float32 [4, 8], P(None, 'tensor'), may hold values from 0.005 to 0.05
- v_exp: float32 [4, 8], P(None, 'tensor'), may hold values from 1 to 10
Outputs:
- new_param: float32 [4, 8192, 1024], P(None, 'dp', 'tensor')
- new_q_m: bfloat16 [4, 8192, 1024], P(None, 'dp', 'tensor')
- new_m_scale: float32 [4], replicated
- new_q_v: bfloat16 [4, 8192, 1024], P(None, 'dp', 'tensor')
- new_v_max: float32 [4, 8], P(None, 'tensor')
- new_v_exp: float32 [4, 8], P(None, 'tensor')
The draws below stay inside these ranges and needn't reach their ends.
All inputs are finite; a program needn't handle non-finite values. Where the reference program divides by a largest or mean magnitude, that divisor is 1e-20 or more.
Results may differ from the reference program's by a relative error of at most 0.001.
Values sent between devices are 32-bit elements; how exact they have to be, the bound alone decides.
A program may use at most 192 MiB of HBM per device.

```python
import math
import jax
import jax.numpy as jnp
from jax import lax

D = 8192
KVW = 1024
HEAD = 128
TENSORS = 4
GROUPS = 8
REPLICAS = 32


def with_spikes(result, rng, source, target, parts, factor):
    def block_of(position):
        return (jnp.arange(result.shape[position]) // (result.shape[position] // parts)).reshape((-1,) + (1,) * (result.ndim - 1 - position))

    one_side = jax.random.permutation(rng, parts)[block_of(target)]
    second = (block_of(target) + parts // 2) % parts
    return jnp.where((block_of(source) == one_side) | (block_of(source) == second), factor * result, result)


def shard_levels(stream_key, dims, split, smallest, largest):
    loudness, own = 1.0, jax.random.fold_in(stream_key, 6)
    for axis_at, shards_of in split:
        steps = jnp.exp(jax.random.uniform(jax.random.fold_in(own, axis_at), (shards_of,), jnp.float32, smallest / len(split), largest / len(split)))
        loudness = loudness * jnp.repeat(steps, dims[axis_at] // shards_of).reshape([-1 if axis == axis_at else 1 for axis in range(len(dims))])
    return loudness


def gaussian(rng, shape, deviation, most, pieces=(), kind=jnp.bfloat16):
    values = jax.random.normal(rng, shape, jnp.float32) * deviation
    if len(pieces) > 0:
        values = shard_levels(rng, shape, pieces, -0.22, 0.18) * values
    return jnp.clip(values, min=-most, max=most).astype(kind)


def heavy_noise(stream_key, shape, scale, most, split, heavy, dtype=jnp.bfloat16):
    values = scale * jax.random.normal(stream_key, shape, jnp.float32)
    if split:
        values = values * shard_levels(stream_key, shape, split, -0.22, 0.18)
    return jnp.clip(with_spikes(values, jax.random.fold_in(stream_key, 3), *heavy), -most, most).astype(dtype)


def setup_inputs(seed: int = 0) -> dict:
    streams_of = jax.random.split(jax.random.key(seed), 8)
    return {
        "grads": heavy_noise(streams_of[0], (REPLICAS, TENSORS, D, KVW), 1.0, 6.0, ((0, 32), (3, 4)), (0, 2, 32, 2.75)),
        "param": gaussian(streams_of[1], (TENSORS, D, KVW), 0.5, 3.0, ((1, 32), (2, 4)), jnp.float32),
        "q_m": jnp.clip(jax.random.uniform(streams_of[2], (TENSORS, D, KVW), jnp.float32, -1.0, 1.0) * shard_levels(streams_of[2], (TENSORS, D, KVW), ((1, 32), (2, 4)), -0.4, 0.0), -1.0, 1.0).astype(jnp.bfloat16),
        "m_scale": jnp.clip(jnp.exp(jax.random.uniform(streams_of[3], (TENSORS,), jnp.float32, math.log(0.02), math.log(0.2))), 0.02, 0.2),
        "q_v": jnp.clip(jnp.exp(math.log(1.0) - 6.9083047 * jax.random.uniform(streams_of[4], (TENSORS, D, KVW), jnp.float32) ** shard_levels(streams_of[4], (TENSORS, D, KVW), ((1, 32), (2, 4)), -0.2, 0.2)), 0.0009994507, 1.0).astype(jnp.bfloat16),
        "v_max": jnp.clip(jnp.exp(math.log(0.05) - 2.3025851 * jax.random.uniform(streams_of[5], (TENSORS, GROUPS), jnp.float32) ** shard_levels(streams_of[5], (TENSORS, GROUPS), ((1, 4),), -0.2, 0.2)), 0.005, 0.05),
        "v_exp": jnp.clip(1.0 + 9.0 * jax.random.uniform(streams_of[6], (TENSORS, GROUPS), jnp.float32) ** shard_levels(streams_of[6], (TENSORS, GROUPS), ((1, 4),), -0.2, 0.2), 1.0, 10.0),
    }


def reference(grads, param, q_m, m_scale, q_v, v_max, v_exp):

    def add_one(index, total):
        return total + lax.dynamic_index_in_dim(grads, index, 0, keepdims=False).astype(jnp.float32)
    summed = lax.fori_loop(0, REPLICAS, add_one, jnp.zeros((TENSORS, D, KVW), jnp.float32))
    grad = (summed / REPLICAS).reshape(TENSORS, D, GROUPS, HEAD)
    m_old = m_scale[:, None, None, None] * q_m.astype(jnp.float32).reshape(TENSORS, D, GROUPS, HEAD)
    stored = q_v.astype(jnp.float32).reshape(TENSORS, D, GROUPS, HEAD)
    v_old = v_max[:, None, :, None] * jnp.exp(jnp.log(stored) / v_exp[:, None, :, None])
    m_new = 0.9 * m_old + 0.1 * grad
    v_new = 0.95 * v_old + 0.05 * grad * grad
    weights = param.reshape(TENSORS, D, GROUPS, HEAD)
    new_param = weights - 0.02 * (m_new / (jnp.sqrt(v_new) + 1e-08) + 0.1 * weights)
    new_m_scale = lax.optimization_barrier(jnp.max(jnp.abs(m_new), axis=(1, 2, 3))) + 1e-06
    new_v_max = lax.optimization_barrier(jnp.max(v_new, axis=(1, 3)))
    v_low = lax.optimization_barrier(jnp.min(v_new, axis=(1, 3)))
    new_v_exp = 12.343 / jnp.maximum(jnp.log(new_v_max / v_low), 1.0)
    new_q_m = (m_new / new_m_scale[:, None, None, None]).astype(jnp.bfloat16)
    new_q_v = jnp.exp(new_v_exp[:, None, :, None] * jnp.log(v_new / new_v_max[:, None, :, None])).astype(jnp.bfloat16)
    shape = (TENSORS, D, KVW)
    return (new_param.reshape(shape), new_q_m.reshape(shape), new_m_scale, new_q_v.reshape(shape), new_v_max, new_v_exp)
```

```python
import jax
import jax.numpy as jnp
from jax import lax
from jax.experimental import pallas as pl
from jax.experimental.pallas import tpu as pltpu
from jax.sharding import Mesh
from jax.sharding import PartitionSpec as P

MESH = pl.DeviceIdType.MESH
DP = ("y", "x", "zl")
TENSOR = ("zh", "core")
ROWS = 256
LANES = 128
SPLIT = (64, 104, 88)
PARTS = ((0, 48), (48, 40))
N = 8
SEMS = 42
LIMIT = 55 * 2**20
ORDER = ("F1y", "F2z", "Z1a", "F2y", "S1", "A3z", "F1x", "F2x", "A1y", "A2y", "Z1b", "E", "A1x", "A2z", "A2x")
LAGS = dict(S1=0, A1y=2, A1x=1, Z1a=2, Z1b=2, F1y=5, F1x=2, A2z=2, A2y=6, A2x=3,
            F2z=4, F2y=8, F2x=6, A3z=6, E=10)


def columns(ref, m):
    t, g = lax.div(m, 2), lax.rem(m, 2)
    return ref.at[t, ..., pl.ds(pl.multiple_of(g * LANES, LANES), LANES)]


def kernel(
    g_hbm, p_hbm, qm_hbm, ms_ref, qv_hbm, vm_ref, ve_ref,
    par, mnew, lv, table,
    G, S0, X0, Y0, Z0, S1b, X1, Y1, Z1, S2, Z2, X2, Y2,
    qm, qv, grad, stat, wide, deep,
    rsem, ssem, gsem, psem, asem, atsem,
):
    y, x, z = lax.axis_index("y"), lax.axis_index("x"), lax.axis_index("zl")
    zh, core = lax.axis_index("zh"), lax.axis_index("core")

    lane = lax.broadcasted_iota(jnp.int32, (1, LANES), 1)

    def step_of(coord, d):
        return lax.rem(coord + (1 if d == 0 else 3), 4)

    def to(axis, d):
        if axis == "zl":
            return {"zl": 1 - z}
        return {axis: step_of(x if axis == "x" else y, d)}

    def remote(m, idx, src, dst, target):
        return pltpu.make_async_remote_copy(
            src_ref=src, dst_ref=dst, send_sem=ssem.at[m, idx], recv_sem=rsem.at[m, idx],
            device_id=target, device_id_type=MESH,
        )

    def load_g(m):
        return pltpu.make_async_copy(columns(g_hbm, m), G.at[m], gsem.at[m])

    def load_state(m):
        return [
            pltpu.make_async_copy(columns(h, m), v.at[m], psem.at[m, i])
            for i, (h, v) in enumerate(((p_hbm, par), (qm_hbm, qm), (qv_hbm, qv)))
        ]

    def local(kind, m, yy, xx, zz):
        if kind == 0:
            return G[m, yy, xx, zz, 0:64, :].astype(jnp.float32)
        if kind == 1:
            return G[m, yy, xx, zz, 64:176, :].astype(jnp.float32)[:104]
        return G[m, yy, xx, zz, 160:256, :].astype(jnp.float32)[8:]

    class Plane:
        def __init__(self, kind, first, second, p, q, stage, bx, by, bz):
            self.kind, self.first, self.second, self.p, self.q = kind, first, second, p, q
            self.stage, self.bx, self.by, self.bz, self.base = stage, bx, by, bz, 13 * kind

        def own(self, m, pp, qq, zz):
            yy, xx = (qq, pp) if self.kind == 0 else (pp, qq)
            return local(self.kind, m, yy, xx, zz)

        def far1(self, m, d):
            return remote(m, self.base + d, self.stage.at[lax.rem(m, 2), 0, d],
                          self.bx.at[m, 0, d], to(self.first, d))

        def own1(self, m, d):
            return remote(m, self.base + 2 + d, self.stage.at[lax.rem(m, 2), 1, d],
                          self.bx.at[m, 1, d], to(self.first, d))

        def acc1(self, m, d):
            return remote(m, self.base + 4 + d, self.bx.at[m, 0, d],
                          self.bx.at[m, 2, d], to(self.first, d))

        def far2(self, m, d):
            return remote(m, self.base + 6 + d, self.bx.at[m, 2, d, lax.rem(self.q + 2, 4)],
                          self.by.at[m, 0, d], to(self.second, d))

        def own2(self, m, d):
            return remote(m, self.base + 8 + d, self.bx.at[m, 2, 1 - d, step_of(self.q, d)],
                          self.by.at[m, 1, d], to(self.second, d))

        def acc2(self, m, d):
            return remote(m, self.base + 10 + d, self.by.at[m, 0, d],
                          self.by.at[m, 2, d], to(self.second, d))

        def last(self, m):
            return remote(m, self.base + 12, self.by.at[m, 2, 1 - z], self.bz.at[m], to("zl", 0))

        def S_far(self, m):
            slot = lax.rem(m, 2)
            for d in range(2):
                for q in range(4):
                    self.stage[slot, 0, d, q] = self.own(m, lax.rem(self.p + 2, 4), q, d)
                self.far1(m, d).start()

        def S_own(self, m):
            slot = lax.rem(m, 2)
            for d in range(2):
                for q in range(4):
                    self.stage[slot, 1, d, q] = self.own(m, step_of(self.p, d), q, 1 - d)
                self.own1(m, d).start()

        def A1(self, m):
            for d in range(2):
                self.far1(m, d).wait_recv()
                for q in range(4):
                    self.bx[m, 0, d, q] += self.own(m, step_of(self.p, d), q, d)
                self.acc1(m, d).start()

        def F1(self, m):
            for d in range(2):
                self.own1(m, d).wait_recv()
                self.acc1(m, d).wait_recv()
            for h in range(2):
                for q in range(4):
                    self.bx[m, 2, h, q] += self.own(m, self.p, q, h) + self.bx[m, 1, 1 - h, q]
            for d in range(2):
                self.far2(m, d).start()
            for d in range(2):
                self.own2(m, d).start()

        def A2(self, m):
            for d in range(2):
                self.far2(m, d).wait_recv()
                self.by[m, 0, d] += self.bx[m, 2, d, step_of(self.q, d)]
                self.acc2(m, d).start()

        def F2(self, m):
            for d in range(2):
                self.own2(m, d).wait_recv()
                self.acc2(m, d).wait_recv()
            for h in range(2):
                self.by[m, 2, h] += self.bx[m, 2, h, self.q] + self.by[m, 1, 1 - h]
            self.last(m).start()

        def total(self, m):
            self.last(m).wait_recv()
            return self.by[m, 2, z] + self.bz[m]

        def staged(self, m):
            return [f(m, d) for f in (self.far1, self.own1) for d in range(2)]

        def unstaged(self, m):
            return [
                f(m, d) for f in (self.acc1, self.far2, self.own2, self.acc2) for d in range(2)
            ] + [self.last(m)]

    class ZFirst:
        def xs(self, j):
            return lax.rem(x + (2, 1, 3, 0)[j], 4)

        def zsend(self, m, j):
            return remote(m, 26 + j, S2.at[lax.rem(m, 2), self.xs(j)], Z2.at[m, self.xs(j)],
                          to("zl", 0))

        def far1(self, m, d):
            return remote(m, 30 + d, Z2.at[m, self.xs(0), pl.ds(2 * d, 2)],
                          X2.at[m, 0, pl.ds(2 * d, 2)], to("x", d))

        def own1(self, m, d):
            return remote(m, 32 + d, Z2.at[m, self.xs(1 + d), pl.ds(2 - 2 * d, 2)],
                          X2.at[m, 1, pl.ds(2 - 2 * d, 2)], to("x", d))

        def acc1(self, m, d):
            return remote(m, 34 + d, X2.at[m, 0, pl.ds(2 * d, 2)], X2.at[m, 2, pl.ds(2 * d, 2)],
                          to("x", d))

        def far2(self, m, d):
            part = pl.ds(*PARTS[d])
            return remote(m, 36 + d, X2.at[m, 2, lax.rem(y + 2, 4), part], Y2.at[m, 0, part],
                          to("y", d))

        def own2(self, m, d):
            part = pl.ds(*PARTS[1 - d])
            return remote(m, 38 + d, X2.at[m, 2, step_of(y, d), part], Y2.at[m, 1, part],
                          to("y", d))

        def acc2(self, m, d):
            part = pl.ds(*PARTS[d])
            return remote(m, 40 + d, Y2.at[m, 0, part], Y2.at[m, 2, part], to("y", d))

        def S(self, m, js):
            slot = lax.rem(m, 2)
            for j in js:
                for yy in range(4):
                    S2[slot, self.xs(j), yy] = local(2, m, yy, self.xs(j), 1 - z)
                self.zsend(m, j).start()

        def Z(self, m, j):
            self.zsend(m, j).wait_recv()
            for yy in range(4):
                Z2[m, self.xs(j), yy] += local(2, m, yy, self.xs(j), z)

        def Z1a(self, m):
            self.Z(m, 0)
            for d in range(2):
                self.far1(m, d).start()
            self.Z(m, 1)
            self.own1(m, 0).start()

        def Z1b(self, m):
            self.Z(m, 2)
            self.own1(m, 1).start()
            self.Z(m, 3)

        def A1(self, m):
            for d in range(2):
                self.far1(m, d).wait_recv()
                for i in range(2):
                    X2[m, 0, 2 * d + i] += Z2[m, self.xs(1 + d), 2 * d + i]
                self.acc1(m, d).start()

        def F1(self, m):
            for d in range(2):
                self.own1(m, d).wait_recv()
                self.acc1(m, d).wait_recv()
            for yy in range(4):
                X2[m, 2, yy] += Z2[m, x, yy] + X2[m, 1, yy]
            for d in range(2):
                self.far2(m, d).start()
            for d in range(2):
                self.own2(m, d).start()

        def A2(self, m):
            for d in range(2):
                self.far2(m, d).wait_recv()
                part = pl.ds(*PARTS[d])
                Y2[m, 0, part] += X2[m, 2, step_of(y, d), part]
                self.acc2(m, d).start()

        def total(self, m):
            for d in range(2):
                self.own2(m, d).wait_recv()
                self.acc2(m, d).wait_recv()
            return X2[m, 2, y] + Y2[m, 1] + Y2[m, 2]

        def staged(self, m):
            return [self.zsend(m, j) for j in range(4)]

        def unstaged(self, m):
            return [
                f(m, d)
                for f in (self.far1, self.own1, self.acc1, self.far2, self.own2, self.acc2)
                for d in range(2)
            ]

    A = Plane(0, "x", "y", x, y, S0, X0, Y0, Z0)
    B = Plane(1, "y", "x", y, x, S1b, X1, Y1, Z1)
    C = ZFirst()

    def begin(m):
        @pl.when(m >= 2)
        def _():
            for c in A.staged(m - 2) + B.staged(m - 2) + C.staged(m - 2):
                c.wait_send()

        load_g(m).wait()

        @pl.when(m + 2 < N)
        def _():
            load_g(m + 2).start()

        for c in load_state(m):
            c.start()
        B.S_far(m)
        A.S_far(m)
        C.S(m, (0,))
        B.S_own(m)
        A.S_own(m)
        C.S(m, (1, 2, 3))

    def update(m):
        r0 = 0
        for color, s in zip((A, B, C), SPLIT):
            grad[r0 : r0 + s] = color.total(m)
            r0 += s
        for c in load_state(m):
            c.wait()
        t, g = lax.div(m, 2), lax.rem(m, 2)
        scale, top = ms_ref[t], vm_ref[g, t]
        inverse = 1.0 / jnp.full((8, LANES), ve_ref[g, t], jnp.float32)[0:1]
        rows = 32

        def body(i, carry):
            hi, lo, peak = carry
            at = pl.ds(pl.multiple_of(i * rows, rows), rows)
            gr = grad[at] * (1.0 / 32)
            m_old = scale * qm[m, at].astype(jnp.float32)
            v_old = top * jnp.exp(jnp.log(qv[m, at].astype(jnp.float32)) * inverse)
            m_new = 0.9 * m_old + 0.1 * gr
            v_new = 0.95 * v_old + 0.05 * gr * gr
            w = par[m, at]
            par[m, at] = w - 0.02 * (m_new / (jnp.sqrt(v_new) + 1e-8) + 0.1 * w)
            mnew[m, at] = m_new
            lv[m, at] = jnp.log(v_new)
            fold = lambda v: v.reshape(rows // 8, 8, LANES)
            return (
                jnp.maximum(hi, jnp.max(fold(v_new), axis=0)),
                jnp.minimum(lo, jnp.min(fold(v_new), axis=0)),
                jnp.maximum(peak, jnp.max(fold(jnp.abs(m_new)), axis=0)),
            )

        start = jnp.zeros((8, LANES), jnp.float32)
        hi, lo, peak = lax.fori_loop(0, ROWS // rows, body, (start, start + 3e38, start))
        row = stat[0:1]
        for i, v in enumerate((hi, -lo, peak)):
            v = jnp.max(jnp.max(v, axis=0, keepdims=True), axis=1, keepdims=True)
            row = jnp.where(lane == 8 * i + 4 * g + t, v, row)
        stat[0:1] = row
        for c in A.unstaged(m) + B.unstaged(m) + C.unstaged(m):
            c.wait_send()

    stat[...] = jnp.full(stat.shape, -3e38, jnp.float32)
    ops = dict(S1=begin, A1y=B.A1, A1x=A.A1, Z1a=C.Z1a, Z1b=C.Z1b, F1y=B.F1, F1x=A.F1,
               A2z=C.A1, A2y=B.A2, A2x=A.A2, F2z=C.F1, F2y=B.F2, F2x=A.F2, A3z=C.A2, E=update)

    flip = lambda v, b: v + b - 2 * b * v
    plane_peers = [
        {"y": lax.rem(y + j, 4), "x": lax.rem(x + k, 4)}
        for j in range(4) for k in range(4) if j or k
    ]
    column_peers = [
        {"zl": flip(z, i & 1), "core": flip(core, i >> 1 & 1), "zh": flip(zh, i >> 2)}
        for i in range(1, 8)
    ]

    load_g(0).start()
    barrier = pltpu.get_barrier_semaphore()
    peers = [to(axis, d) for axis in ("x", "y") for d in range(2)] + column_peers
    for peer in peers:
        pl.semaphore_signal(barrier, inc=1, device_id=peer, device_id_type=MESH)
    load_g(1).start()
    pl.semaphore_wait(barrier, len(peers))

    def step(k, _):
        for name in ORDER:
            m = k - LAGS[name]
            pl.when((m >= 0) & (m < N))(lambda f=ops[name], m=m: f(m))
        return 0

    lax.fori_loop(0, N + max(LAGS.values()), step, 0)

    first = 0
    for who, buf in ((plane_peers, wide), (column_peers, deep)):
        copies = [
            pltpu.make_async_remote_copy(
                src_ref=stat.at[pl.ds(8 * (first > 0), 1)], dst_ref=buf.at[pl.ds(i, 1)],
                send_sem=atsem.at[first + i], recv_sem=asem.at[first + i],
                device_id=peer, device_id_type=MESH,
            )
            for i, peer in enumerate(who)
        ]
        for c in copies:
            c.start()
        mine = stat[8:9] if first else stat[0:1]
        buf[len(who) : len(who) + 1] = mine
        for c in copies:
            c.wait_recv()
        most = jnp.max(buf[...], axis=0, keepdims=True)
        if first == 0:
            stat[8:9] = most
        else:
            table[...] = jnp.where(lane < 16, jnp.maximum(mine, buf[0:1]), most)
        for c in copies:
            c.wait_send()
        first += len(who)
    for m in (N - 2, N - 1):
        for c in A.staged(m) + B.staged(m) + C.staged(m):
            c.wait_send()


def finish(par, mnew, lv, table, np_hbm, nqm_hbm, nms_ref, nqv_hbm, nvm_ref, nve_ref, qmo, qvo, sem):
    def store_out(m, i):
        h, v = ((np_hbm, par), (nqm_hbm, qmo), (nqv_hbm, qvo))[i]
        return pltpu.make_async_copy(v.at[m], columns(h, m), sem.at[m, i])

    for m in range(N):
        store_out(m, 0).start()
    row = table[...]
    lane = lax.broadcasted_iota(jnp.int32, (1, LANES), 1)
    left = lambda v, k: pltpu.roll(v, LANES - k, 1)
    low, peak = -left(row, 8), left(row, 16)
    scale = jnp.maximum(peak, left(peak, 4)) + 1e-6
    new_exp = 12.343 / jnp.maximum(jnp.log(row / low), 1.0)
    log_top, inverse = jnp.log(row), 1.0 / scale
    pick = lambda v, i: jnp.max(jnp.where(lane == i, v, -3e38), axis=1, keepdims=True)
    for m in range(N):
        t, g = m // 2, m % 2
        qmo[m] = (mnew[m] * pick(inverse, t)).astype(jnp.bfloat16)
        store_out(m, 1).start()
        e, top = pick(new_exp, 4 * g + t), pick(log_top, 4 * g + t)
        qvo[m] = jnp.exp(e * (lv[m] - top)).astype(jnp.bfloat16)
        store_out(m, 2).start()
    nms_ref[...] = scale[:, 0:4]
    for g in range(2):
        nvm_ref[g : g + 1, :] = left(row, 4 * g)[:, 0:4] if g else row[:, 0:4]
        nve_ref[g : g + 1, :] = left(new_exp, 4 * g)[:, 0:4] if g else new_exp[:, 0:4]
    for m in range(N):
        for i in range(3):
            store_out(m, i).wait()


def on_device(grads, param, q_m, m_scale, q_v, v_max, v_exp):
    f32, bf16 = jnp.float32, jnp.bfloat16
    a, b, c = SPLIT
    plane = lambda s: [
        pltpu.VMEM((2, 2, 2, 4, s, LANES), f32),
        pltpu.VMEM((N, 3, 2, 4, s, LANES), f32),
        pltpu.VMEM((N, 3, 2, s, LANES), f32),
        pltpu.VMEM((N, s, LANES), f32),
    ]
    block = lambda kind: pltpu.VMEM((N, ROWS, LANES), kind)
    anywhere, smem = pl.BlockSpec(memory_space=pl.ANY), pl.BlockSpec(memory_space=pltpu.SMEM)
    vmem = pl.BlockSpec(memory_space=pltpu.VMEM)
    kept = pl.pallas_call(
        kernel,
        out_shape=(block(f32), block(f32), block(f32), pltpu.VMEM((1, LANES), f32)),
        in_specs=[anywhere, anywhere, anywhere, smem, anywhere, smem, smem],
        out_specs=(vmem,) * 4,
        scratch_shapes=[
            pltpu.VMEM((N, 4, 4, 2, ROWS, LANES), bf16),
            *plane(a),
            *plane(b),
            pltpu.VMEM((2, 4, 4, c, LANES), f32),
            pltpu.VMEM((N, 4, 4, c, LANES), f32),
            pltpu.VMEM((N, 3, 4, c, LANES), f32),
            pltpu.VMEM((N, 3, c, LANES), f32),
            block(bf16), block(bf16),
            pltpu.VMEM((ROWS, LANES), f32),
            pltpu.VMEM((16, LANES), f32),
            pltpu.VMEM((16, LANES), f32),
            pltpu.VMEM((8, LANES), f32),
            pltpu.SemaphoreType.DMA((N, SEMS)),
            pltpu.SemaphoreType.DMA((N, SEMS)),
            pltpu.SemaphoreType.DMA((N,)),
            pltpu.SemaphoreType.DMA((N, 3)),
            pltpu.SemaphoreType.DMA((22,)),
            pltpu.SemaphoreType.DMA((22,)),
        ],
        compiler_params=pltpu.CompilerParams(
            collective_id=0, has_side_effects=True, vmem_limit_bytes=LIMIT
        ),
    )(grads[0].reshape(4, 4, 4, 2, ROWS, 2 * LANES), param, q_m, m_scale, q_v, v_max.T, v_exp.T)
    small = lambda rows: jax.ShapeDtypeStruct((rows, 4), f32)
    new_param, new_q_m, ms, new_q_v, vm, ve = pl.pallas_call(
        finish,
        out_shape=(
            jax.ShapeDtypeStruct(param.shape, f32),
            jax.ShapeDtypeStruct(q_m.shape, bf16),
            small(1),
            jax.ShapeDtypeStruct(q_v.shape, bf16),
            small(2),
            small(2),
        ),
        in_specs=[vmem] * 4,
        out_specs=(anywhere, anywhere, vmem, anywhere, vmem, vmem),
        scratch_shapes=[block(bf16), block(bf16), pltpu.SemaphoreType.DMA((N, 3))],
        compiler_params=pltpu.CompilerParams(vmem_limit_bytes=8 * 2**20),
    )(*kept)
    return new_param, new_q_m, ms[0], new_q_v, vm.T, ve.T


def solution(mesh):
    split = Mesh(mesh.devices.reshape(2, 2, 4, 4, 2), TENSOR + DP)
    return jax.shard_map(
        on_device,
        mesh=split,
        in_specs=(
            P(DP, None, None, TENSOR),
            P(None, DP, TENSOR),
            P(None, DP, TENSOR),
            P(),
            P(None, DP, TENSOR),
            P(None, TENSOR),
            P(None, TENSOR),
        ),
        out_specs=(
            P(None, DP, TENSOR),
            P(None, DP, TENSOR),
            P(),
            P(None, DP, TENSOR),
            P(None, TENSOR),
            P(None, TENSOR),
        ),
        check_vma=False,
    )
```

```python
import jax
import jax.numpy as jnp
from jax import lax
from jax.experimental import pallas as pl
from jax.experimental.pallas import tpu as pltpu
from jax.sharding import Mesh
from jax.sharding import PartitionSpec as P

MESH = pl.DeviceIdType.MESH
DP = ("y", "x", "zl")
TENSOR = ("zh", "core")
ROWS = 256
LANES = 128
SPLIT = (64, 104, 88)
PARTS = ((0, 48), (48, 40))
N = 8
SEMS = 42
LIMIT = 55 * 2**20
ORDER = ('F2z', 'F2y', 'A2y', 'A1x', 'EA', 'F1x', 'Z1b', 'EC', 'S1', 'A1y', 'A2z', 'F2x', 'F1y', 'A2x', 'A3z', 'EB', 'Z1a')
LAGS = {'S1': 0, 'A1y': 1, 'A1x': 2, 'Z1a': 2, 'Z1b': 3, 'F1y': 2, 'F1x': 3, 'A2z': 6, 'A2y': 4, 'A2x': 7, 'F2z': 15, 'F2y': 8, 'F2x': 16, 'A3z': 23, 'EA': 26, 'EB': 16, 'EC': 32}


def columns(ref, m):
    t, g = lax.div(m, 2), lax.rem(m, 2)
    return ref.at[t, ..., pl.ds(pl.multiple_of(g * LANES, LANES), LANES)]


def kernel(
    g_hbm, p_hbm, qm_hbm, ms_ref, qv_hbm, vm_ref, ve_ref,
    par, mnew, lv, table,
    G, S0, X0, Y0, Z0, S1b, X1, Y1, Z1, S2, Z2, X2, Y2,
    qm, qv, stat, wide, deep,
    rsem, ssem, gsem, psem, asem, atsem,
):
    y, x, z = lax.axis_index("y"), lax.axis_index("x"), lax.axis_index("zl")
    zh, core = lax.axis_index("zh"), lax.axis_index("core")

    lane = lax.broadcasted_iota(jnp.int32, (1, LANES), 1)

    def step_of(coord, d):
        return lax.rem(coord + (1 if d == 0 else 3), 4)

    def place(m):
        s = lax.rem(m, 2)
        return x + s * (y - x), y + s * (x - y)

    def to(m, axis, d):
        if axis == "z":
            return {"zl": 1 - z}
        s = lax.rem(m, 2)
        s = s if axis == "u" else 1 - s
        return {"x": x + (1 - s) * (step_of(x, d) - x), "y": y + s * (step_of(y, d) - y)}

    def remote(m, idx, src, dst, target):
        return pltpu.make_async_remote_copy(
            src_ref=src, dst_ref=dst, send_sem=ssem.at[m, idx], recv_sem=rsem.at[m, idx],
            device_id=target, device_id_type=MESH,
        )

    def load_g(m):
        return pltpu.make_async_copy(columns(g_hbm, m), G.at[m], gsem.at[m])

    def load_state(m):
        return [
            pltpu.make_async_copy(columns(h, m), v.at[m], psem.at[m, i])
            for i, (h, v) in enumerate(((p_hbm, par), (qm_hbm, qm), (qv_hbm, qv)))
        ]

    def local(kind, m, uu, vv, zz):
        s = lax.rem(m, 2)
        yy, xx = vv + s * (uu - vv), uu + s * (vv - uu)
        if kind == 0:
            return G[m, yy, xx, zz, 0:64, :].astype(jnp.float32)
        if kind == 1:
            return G[m, yy, xx, zz, 64:176, :].astype(jnp.float32)[:104]
        return G[m, yy, xx, zz, 160:256, :].astype(jnp.float32)[8:]

    class Plane:
        def __init__(self, kind, first, second, stage, bx, by, bz):
            self.kind, self.first, self.second = kind, first, second
            self.stage, self.bx, self.by, self.bz, self.base = stage, bx, by, bz, 13 * kind

        def own(self, m, pp, qq, zz):
            uu, vv = (pp, qq) if self.first == "u" else (qq, pp)
            return local(self.kind, m, uu, vv, zz)

        def at(self, m):
            u, v = place(m)
            return (u, v) if self.first == "u" else (v, u)

        def far1(self, m, d):
            return remote(m, self.base + d, self.stage.at[lax.rem(m, 2), 0, d],
                          self.bx.at[m, 0, d], to(m, self.first, d))

        def own1(self, m, d):
            return remote(m, self.base + 2 + d, self.stage.at[lax.rem(m, 2), 1, d],
                          self.bx.at[m, 1, d], to(m, self.first, d))

        def acc1(self, m, d):
            return remote(m, self.base + 4 + d, self.bx.at[m, 0, d],
                          self.bx.at[m, 2, d], to(m, self.first, d))

        def far2(self, m, d):
            q = self.at(m)[1]
            return remote(m, self.base + 6 + d, self.bx.at[m, 2, d, lax.rem(q + 2, 4)],
                          self.by.at[m, 0, d], to(m, self.second, d))

        def own2(self, m, d):
            q = self.at(m)[1]
            return remote(m, self.base + 8 + d, self.bx.at[m, 2, 1 - d, step_of(q, d)],
                          self.by.at[m, 1, d], to(m, self.second, d))

        def acc2(self, m, d):
            return remote(m, self.base + 10 + d, self.by.at[m, 0, d],
                          self.by.at[m, 2, d], to(m, self.second, d))

        def last(self, m):
            return remote(m, self.base + 12, self.by.at[m, 2, 1 - z], self.bz.at[m], to(m, "z", 0))

        def S_far(self, m):
            slot, p = lax.rem(m, 2), self.at(m)[0]
            for d in range(2):
                for q in range(4):
                    self.stage[slot, 0, d, q] = self.own(m, lax.rem(p + 2, 4), q, d)
                self.far1(m, d).start()

        def S_own(self, m):
            slot, p = lax.rem(m, 2), self.at(m)[0]
            for d in range(2):
                for q in range(4):
                    self.stage[slot, 1, d, q] = self.own(m, step_of(p, d), q, 1 - d)
                self.own1(m, d).start()

        def A1(self, m):
            p = self.at(m)[0]
            for d in range(2):
                self.far1(m, d).wait_recv()
                for q in range(4):
                    self.bx[m, 0, d, q] += self.own(m, step_of(p, d), q, d)
                self.acc1(m, d).start()

        def F1(self, m):
            p = self.at(m)[0]
            for d in range(2):
                self.own1(m, d).wait_recv()
                self.acc1(m, d).wait_recv()
            for h in range(2):
                for q in range(4):
                    self.bx[m, 2, h, q] += self.own(m, p, q, h) + self.bx[m, 1, 1 - h, q]
            for d in range(2):
                self.far2(m, d).start()
            for d in range(2):
                self.own2(m, d).start()

        def A2(self, m):
            q = self.at(m)[1]
            for d in range(2):
                self.far2(m, d).wait_recv()
                self.by[m, 0, d] += self.bx[m, 2, d, step_of(q, d)]
                self.acc2(m, d).start()

        def F2(self, m):
            q = self.at(m)[1]
            for d in range(2):
                self.own2(m, d).wait_recv()
                self.acc2(m, d).wait_recv()
            for h in range(2):
                self.by[m, 2, h] += self.bx[m, 2, h, q] + self.by[m, 1, 1 - h]
            self.last(m).start()

        def arrive(self, m):
            self.last(m).wait_recv()

        def total(self, m, rows):
            return self.by[m, 2, z, rows] + self.bz[m, rows]

        def staged(self, m):
            return [f(m, d) for f in (self.far1, self.own1) for d in range(2)]

        def unstaged(self, m):
            return [
                f(m, d) for f in (self.acc1, self.far2, self.own2, self.acc2) for d in range(2)
            ] + [self.last(m)]

    class ZFirst:
        def us(self, m, j):
            return lax.rem(place(m)[0] + (2, 1, 3, 0)[j], 4)

        def zsend(self, m, j):
            return remote(m, 26 + j, S2.at[lax.rem(m, 2), self.us(m, j)], Z2.at[m, self.us(m, j)],
                          to(m, "z", 0))

        def far1(self, m, d):
            return remote(m, 30 + d, Z2.at[m, self.us(m, 0), pl.ds(2 * d, 2)],
                          X2.at[m, 0, pl.ds(2 * d, 2)], to(m, "u", d))

        def own1(self, m, d):
            return remote(m, 32 + d, Z2.at[m, self.us(m, 1 + d), pl.ds(2 - 2 * d, 2)],
                          X2.at[m, 1, pl.ds(2 - 2 * d, 2)], to(m, "u", d))

        def acc1(self, m, d):
            return remote(m, 34 + d, X2.at[m, 0, pl.ds(2 * d, 2)], X2.at[m, 2, pl.ds(2 * d, 2)],
                          to(m, "u", d))

        def far2(self, m, d):
            part = pl.ds(*PARTS[d])
            return remote(m, 36 + d, X2.at[m, 2, lax.rem(place(m)[1] + 2, 4), part],
                          Y2.at[m, 0, part], to(m, "v", d))

        def own2(self, m, d):
            part = pl.ds(*PARTS[1 - d])
            return remote(m, 38 + d, X2.at[m, 2, step_of(place(m)[1], d), part],
                          Y2.at[m, 1, part], to(m, "v", d))

        def acc2(self, m, d):
            part = pl.ds(*PARTS[d])
            return remote(m, 40 + d, Y2.at[m, 0, part], Y2.at[m, 2, part], to(m, "v", d))

        def S(self, m, js):
            slot = lax.rem(m, 2)
            for j in js:
                for v in range(4):
                    S2[slot, self.us(m, j), v] = local(2, m, self.us(m, j), v, 1 - z)
                self.zsend(m, j).start()

        def Z(self, m, j):
            self.zsend(m, j).wait_recv()
            for v in range(4):
                Z2[m, self.us(m, j), v] += local(2, m, self.us(m, j), v, z)

        def Z1a(self, m):
            self.Z(m, 0)
            for d in range(2):
                self.far1(m, d).start()
            self.Z(m, 1)
            self.own1(m, 0).start()

        def Z1b(self, m):
            self.Z(m, 2)
            self.own1(m, 1).start()
            self.Z(m, 3)

        def A1(self, m):
            for d in range(2):
                self.far1(m, d).wait_recv()
                for i in range(2):
                    X2[m, 0, 2 * d + i] += Z2[m, self.us(m, 1 + d), 2 * d + i]
                self.acc1(m, d).start()

        def F1(self, m):
            for d in range(2):
                self.own1(m, d).wait_recv()
                self.acc1(m, d).wait_recv()
            for v in range(4):
                X2[m, 2, v] += Z2[m, place(m)[0], v] + X2[m, 1, v]
            for d in range(2):
                self.far2(m, d).start()
            for d in range(2):
                self.own2(m, d).start()

        def A2(self, m):
            for d in range(2):
                self.far2(m, d).wait_recv()
                part = pl.ds(*PARTS[d])
                Y2[m, 0, part] += X2[m, 2, step_of(place(m)[1], d), part]
                self.acc2(m, d).start()

        def arrive(self, m):
            for d in range(2):
                self.own2(m, d).wait_recv()
                self.acc2(m, d).wait_recv()

        def total(self, m, rows):
            return X2[m, 2, place(m)[1], rows] + Y2[m, 1, rows] + Y2[m, 2, rows]

        def staged(self, m):
            return [self.zsend(m, j) for j in range(4)]

        def unstaged(self, m):
            return [
                f(m, d)
                for f in (self.far1, self.own1, self.acc1, self.far2, self.own2, self.acc2)
                for d in range(2)
            ]

    A = Plane(0, "u", "v", S0, X0, Y0, Z0)
    B = Plane(1, "v", "u", S1b, X1, Y1, Z1)
    C = ZFirst()

    def begin(m):
        @pl.when(m >= 2)
        def _():
            for c in A.staged(m - 2) + B.staged(m - 2) + C.staged(m - 2):
                c.wait_send()

        load_g(m).wait()

        @pl.when(m + 2 < N)
        def _():
            load_g(m + 2).start()

        B.S_far(m)
        A.S_far(m)
        C.S(m, (0,))
        B.S_own(m)
        A.S_own(m)
        C.S(m, (1, 2, 3))
        for c in load_state(m):
            c.wait()

        @pl.when(m + 1 < N)
        def _():
            for c in load_state(m + 1):
                c.start()

    def update(m, color, r0, size):
        color.arrive(m)
        t, g = lax.div(m, 2), lax.rem(m, 2)
        scale, top = ms_ref[t], vm_ref[g, t]
        inverse = 1.0 / jnp.full((8, LANES), ve_ref[g, t], jnp.float32)[0:1]
        hi = peak = jnp.zeros((8, LANES), jnp.float32)
        lo = hi + 3e38
        at = r0
        while at < r0 + size:
            base = at // 16 * 16
            rows = min(base + 32 if base == at else base + 16, r0 + size) - at
            here = pl.ds(at, rows)
            half = lambda ref: ref[m, base : base + 32 if rows > 16 else base + 16].astype(
                jnp.float32
            )[at - base : at - base + rows]
            gr = color.total(m, pl.ds(at - r0, rows)) * (1.0 / 32)
            m_old = scale * half(qm)
            v_old = top * jnp.exp(jnp.log(half(qv)) * inverse)
            m_new = 0.9 * m_old + 0.1 * gr
            v_new = 0.95 * v_old + 0.05 * gr * gr
            w = par[m, here]
            par[m, here] = w - 0.02 * (m_new / (jnp.sqrt(v_new) + 1e-8) + 0.1 * w)
            mnew[m, here] = m_new
            lv[m, here] = jnp.log(v_new)
            fold = lambda v: v.reshape(rows // 8, 8, LANES)
            hi = jnp.maximum(hi, jnp.max(fold(v_new), axis=0))
            lo = jnp.minimum(lo, jnp.min(fold(v_new), axis=0))
            peak = jnp.maximum(peak, jnp.max(fold(jnp.abs(m_new)), axis=0))
            at += rows
        row = stat[0:1]
        for i, v in enumerate((hi, -lo, peak)):
            v = jnp.max(jnp.max(v, axis=0, keepdims=True), axis=1, keepdims=True)
            row = jnp.where(lane == 8 * i + 4 * g + t, jnp.maximum(row, v), row)
        stat[0:1] = row

    def drain(m):
        for c in A.unstaged(m) + B.unstaged(m) + C.unstaged(m):
            c.wait_send()

    def update_c(m):
        pl.when(m >= 1)(lambda: drain(m - 1))
        update(m, C, 168, 88)

    stat[...] = jnp.full(stat.shape, -3e38, jnp.float32)
    ops = dict(S1=begin, A1y=B.A1, A1x=A.A1, Z1a=C.Z1a, Z1b=C.Z1b, F1y=B.F1, F1x=A.F1,
               A2z=C.A1, A2y=B.A2, A2x=A.A2, F2z=C.F1, F2y=B.F2, F2x=A.F2, A3z=C.A2,
               EA=lambda m: update(m, A, 0, 64), EB=lambda m: update(m, B, 64, 104), EC=update_c)
    assert all(LAGS["EC"] + 1 > v for v in LAGS.values())

    flip = lambda v, b: v + b - 2 * b * v
    plane_peers = [
        {"y": lax.rem(y + j, 4), "x": lax.rem(x + k, 4)}
        for j in range(4) for k in range(4) if j or k
    ]
    column_peers = [
        {"zl": flip(z, i & 1), "core": flip(core, i >> 1 & 1), "zh": flip(zh, i >> 2)}
        for i in range(1, 8)
    ]

    load_g(0).start()
    barrier = pltpu.get_barrier_semaphore()
    peers = [to(0, axis, d) for axis in ("u", "v") for d in range(2)] + column_peers
    for peer in peers:
        pl.semaphore_signal(barrier, inc=1, device_id=peer, device_id_type=MESH)
    load_g(1).start()
    pl.semaphore_wait(barrier, len(peers))
    for c in load_state(0):
        c.start()

    def step(k, _):
        for name in ORDER:
            m = k - LAGS[name]
            pl.when((m >= 0) & (m < N))(lambda f=ops[name], m=m: f(m))
        return 0

    lax.fori_loop(0, N + max(LAGS.values()), step, 0)

    first = 0
    for who, buf in ((plane_peers, wide), (column_peers, deep)):
        copies = [
            pltpu.make_async_remote_copy(
                src_ref=stat.at[pl.ds(8 * (first > 0), 1)], dst_ref=buf.at[pl.ds(i, 1)],
                send_sem=atsem.at[first + i], recv_sem=asem.at[first + i],
                device_id=peer, device_id_type=MESH,
            )
            for i, peer in enumerate(who)
        ]
        for c in copies:
            c.start()
        mine = stat[8:9] if first else stat[0:1]
        buf[len(who) : len(who) + 1] = mine
        if first == 0:
            drain(N - 1)
            for m in (N - 2, N - 1):
                for c in A.staged(m) + B.staged(m) + C.staged(m):
                    c.wait_send()
        for c in copies:
            c.wait_recv()
        most = jnp.max(buf[...], axis=0, keepdims=True)
        if first == 0:
            stat[8:9] = most
        else:
            table[...] = jnp.where(lane < 16, jnp.maximum(mine, buf[0:1]), most)
        for c in copies:
            c.wait_send()
        first += len(who)


def finish(par, mnew, lv, table, np_hbm, nqm_hbm, nms_ref, nqv_hbm, nvm_ref, nve_ref, qmo, qvo, sem):
    def store_out(m, i):
        h, v = ((np_hbm, par), (nqm_hbm, qmo), (nqv_hbm, qvo))[i]
        return pltpu.make_async_copy(v.at[m], columns(h, m), sem.at[m, i])

    for m in range(N):
        store_out(m, 0).start()
    row = table[...]
    lane = lax.broadcasted_iota(jnp.int32, (1, LANES), 1)
    left = lambda v, k: pltpu.roll(v, LANES - k, 1)
    low, peak = -left(row, 8), left(row, 16)
    scale = jnp.maximum(peak, left(peak, 4)) + 1e-6
    new_exp = 12.343 / jnp.maximum(jnp.log(row / low), 1.0)
    log_top, inverse = jnp.log(row), 1.0 / scale
    pick = lambda v, i: jnp.max(jnp.where(lane == i, v, -3e38), axis=1, keepdims=True)
    for m in range(N):
        t, g = m // 2, m % 2
        qmo[m] = (mnew[m] * pick(inverse, t)).astype(jnp.bfloat16)
        store_out(m, 1).start()
        e, top = pick(new_exp, 4 * g + t), pick(log_top, 4 * g + t)
        qvo[m] = jnp.exp(e * (lv[m] - top)).astype(jnp.bfloat16)
        store_out(m, 2).start()
    nms_ref[...] = scale[:, 0:4]
    for g in range(2):
        nvm_ref[g : g + 1, :] = left(row, 4 * g)[:, 0:4] if g else row[:, 0:4]
        nve_ref[g : g + 1, :] = left(new_exp, 4 * g)[:, 0:4] if g else new_exp[:, 0:4]
    for m in range(N):
        for i in range(3):
            store_out(m, i).wait()


def on_device(grads, param, q_m, m_scale, q_v, v_max, v_exp):
    f32, bf16 = jnp.float32, jnp.bfloat16
    a, b, c = SPLIT
    plane = lambda s: [
        pltpu.VMEM((2, 2, 2, 4, s, LANES), f32),
        pltpu.VMEM((N, 3, 2, 4, s, LANES), f32),
        pltpu.VMEM((N, 3, 2, s, LANES), f32),
        pltpu.VMEM((N, s, LANES), f32),
    ]
    block = lambda kind: pltpu.VMEM((N, ROWS, LANES), kind)
    anywhere, smem = pl.BlockSpec(memory_space=pl.ANY), pl.BlockSpec(memory_space=pltpu.SMEM)
    vmem = pl.BlockSpec(memory_space=pltpu.VMEM)
    kept = pl.pallas_call(
        kernel,
        out_shape=(block(f32), block(f32), block(f32), pltpu.VMEM((1, LANES), f32)),
        in_specs=[anywhere, anywhere, anywhere, smem, anywhere, smem, smem],
        out_specs=(vmem,) * 4,
        scratch_shapes=[
            pltpu.VMEM((N, 4, 4, 2, ROWS, LANES), bf16),
            *plane(a),
            *plane(b),
            pltpu.VMEM((2, 4, 4, c, LANES), f32),
            pltpu.VMEM((N, 4, 4, c, LANES), f32),
            pltpu.VMEM((N, 3, 4, c, LANES), f32),
            pltpu.VMEM((N, 3, c, LANES), f32),
            block(bf16), block(bf16),
            pltpu.VMEM((16, LANES), f32),
            pltpu.VMEM((16, LANES), f32),
            pltpu.VMEM((8, LANES), f32),
            pltpu.SemaphoreType.DMA((N, SEMS)),
            pltpu.SemaphoreType.DMA((N, SEMS)),
            pltpu.SemaphoreType.DMA((N,)),
            pltpu.SemaphoreType.DMA((N, 3)),
            pltpu.SemaphoreType.DMA((22,)),
            pltpu.SemaphoreType.DMA((22,)),
        ],
        compiler_params=pltpu.CompilerParams(
            collective_id=0, has_side_effects=True, vmem_limit_bytes=LIMIT
        ),
    )(grads[0].reshape(4, 4, 4, 2, ROWS, 2 * LANES), param, q_m, m_scale, q_v, v_max.T, v_exp.T)
    small = lambda rows: jax.ShapeDtypeStruct((rows, 4), f32)
    new_param, new_q_m, ms, new_q_v, vm, ve = pl.pallas_call(
        finish,
        out_shape=(
            jax.ShapeDtypeStruct(param.shape, f32),
            jax.ShapeDtypeStruct(q_m.shape, bf16),
            small(1),
            jax.ShapeDtypeStruct(q_v.shape, bf16),
            small(2),
            small(2),
        ),
        in_specs=[vmem] * 4,
        out_specs=(anywhere, anywhere, vmem, anywhere, vmem, vmem),
        scratch_shapes=[block(bf16), block(bf16), pltpu.SemaphoreType.DMA((N, 3))],
        compiler_params=pltpu.CompilerParams(vmem_limit_bytes=8 * 2**20),
    )(*kept)
    return new_param, new_q_m, ms[0], new_q_v, vm.T, ve.T


def solution(mesh):
    split = Mesh(mesh.devices.reshape(2, 2, 4, 4, 2), TENSOR + DP)
    return jax.shard_map(
        on_device,
        mesh=split,
        in_specs=(
            P(DP, None, None, TENSOR),
            P(None, DP, TENSOR),
            P(None, DP, TENSOR),
            P(),
            P(None, DP, TENSOR),
            P(None, TENSOR),
            P(None, TENSOR),
        ),
        out_specs=(
            P(None, DP, TENSOR),
            P(None, DP, TENSOR),
            P(),
            P(None, DP, TENSOR),
            P(None, TENSOR),
            P(None, TENSOR),
        ),
        check_vma=False,
    )
```

```python
import jax
import jax.numpy as jnp
from jax import lax
from jax.experimental import pallas as pl
from jax.experimental.pallas import tpu as pltpu
from jax.sharding import Mesh
from jax.sharding import PartitionSpec as P

MESH = pl.DeviceIdType.MESH
DP = ("y", "x", "zl")
TENSOR = ("zh", "core")
ROWS = 256
LANES = 128
SPLIT = (64, 104, 88)
PARTS = ((0, 48), (48, 40))
LOADS = ((64, 112), (0, 64), (176, 80))
N = 8
SEMS = 24
LIMIT = 55 * 2**20
ORDER = ('A1y', 'A2z', 'F2y', 'F2x', 'EC', 'EA', 'A1x', 'A3z', 'F2z', 'F1y', 'A2x', 'A2y', 'Z1a', 'F1x', 'Z1b', 'EB', 'S1')
LAGS = {'S1': 0, 'A1y': 2, 'A1x': 2, 'Z1a': 3, 'Z1b': 4, 'F1y': 3, 'F1x': 3, 'A2z': 7, 'A2y': 4, 'A2x': 8, 'F2z': 20, 'F2y': 8, 'F2x': 22, 'A3z': 34, 'EA': 36, 'EB': 22, 'EC': 51}


def columns(ref, m):
    t, g = lax.div(m, 2), lax.rem(m, 2)
    return ref.at[t, ..., pl.ds(pl.multiple_of(g * LANES, LANES), LANES)]


def kernel(
    g_hbm, p_hbm, qm_hbm, ms_hbm, qv_hbm, vm_hbm, ve_hbm,
    par, mnew, lv, table,
    G, S0, X0, Y0, Z0, S1b, X1, Y1, Z1, S2, Z2, X2, Y2,
    qm, qv, stat, wide, deep, ms_ref, vm_ref, ve_ref,
    rsem, ssem, stsem, gsem, psem, asem, atsem, csem,
):
    y, x, z = lax.axis_index("y"), lax.axis_index("x"), lax.axis_index("zl")
    zh, core = lax.axis_index("zh"), lax.axis_index("core")

    lane = lax.broadcasted_iota(jnp.int32, (1, LANES), 1)

    def step_of(coord, d):
        return lax.rem(coord + (1 if d == 0 else 3), 4)

    def place(m):
        s = lax.rem(m, 2)
        return x + s * (y - x), y + s * (x - y)

    def to(m, axis, d):
        if axis == "z":
            return {"zl": 1 - z}
        s = lax.rem(m, 2)
        s = s if axis == "u" else 1 - s
        return {"x": x + (1 - s) * (step_of(x, d) - x), "y": y + s * (step_of(y, d) - y)}

    def remote(m, idx, src, dst, target, staged=None):
        sent = ssem.at[m] if staged is None else stsem.at[lax.rem(m, 2), staged]
        return pltpu.make_async_remote_copy(
            src_ref=src, dst_ref=dst, send_sem=sent, recv_sem=rsem.at[m, idx],
            device_id=target, device_id_type=MESH,
        )

    def arrived(m, idx, block):
        remote(m, idx, block, block, to(m, "u", 0)).wait_recv()

    def left(m, block, staged=None):
        remote(m, 0, block, block, to(m, "u", 0), staged).wait_send()

    def load_g(m, i):
        rows = pl.ds(*LOADS[i])
        return pltpu.make_async_copy(
            columns(g_hbm, m).at[:, :, :, rows], G.at[m, :, :, :, rows], gsem.at[lax.rem(m, 2), i]
        )

    scalars = [
        pltpu.make_async_copy(h, v, csem.at[i])
        for i, (h, v) in enumerate(((ms_hbm, ms_ref), (vm_hbm, vm_ref), (ve_hbm, ve_ref)))
    ]

    def load_state(m):
        return [
            pltpu.make_async_copy(columns(h, m), v.at[m], psem.at[i])
            for i, (h, v) in enumerate(((p_hbm, par), (qm_hbm, qm), (qv_hbm, qv)))
        ]

    def local(kind, m, uu, vv, zz):
        s = lax.rem(m, 2)
        yy, xx = vv + s * (uu - vv), uu + s * (vv - uu)
        if kind == 0:
            return G[m, yy, xx, zz, 0:64, :].astype(jnp.float32)
        if kind == 1:
            return G[m, yy, xx, zz, 64:176, :].astype(jnp.float32)[:104]
        return G[m, yy, xx, zz, 160:256, :].astype(jnp.float32)[8:]

    class Plane:
        def __init__(self, kind, first, second, stage, bx, by, bz):
            self.kind, self.first, self.second = kind, first, second
            self.stage, self.bx, self.by, self.bz, self.base = stage, bx, by, bz, 7 * kind

        def own(self, m, pp, qq, zz):
            uu, vv = (pp, qq) if self.first == "u" else (qq, pp)
            return local(self.kind, m, uu, vv, zz)

        def at(self, m):
            u, v = place(m)
            return (u, v) if self.first == "u" else (v, u)

        def far1(self, m, d):
            return remote(m, self.base + d, self.stage.at[lax.rem(m, 2), 0, d],
                          self.bx.at[m, 0, d], to(m, self.first, d), self.kind)

        def own1(self, m, d):
            return remote(m, self.base + 2, self.stage.at[lax.rem(m, 2), 1, d],
                          self.bx.at[m, 1, d], to(m, self.first, d), self.kind)

        def acc1(self, m, d):
            return remote(m, self.base + 2, self.bx.at[m, 0, d],
                          self.bx.at[m, 2, d], to(m, self.first, d))

        def far2(self, m, d):
            q = self.at(m)[1]
            return remote(m, self.base + 3 + d, self.bx.at[m, 2, d, lax.rem(q + 2, 4)],
                          self.by.at[m, 0, d], to(m, self.second, d))

        def own2(self, m, d):
            q = self.at(m)[1]
            return remote(m, self.base + 5, self.bx.at[m, 2, 1 - d, step_of(q, d)],
                          self.by.at[m, 1, d], to(m, self.second, d))

        def acc2(self, m, d):
            return remote(m, self.base + 5, self.by.at[m, 0, d],
                          self.by.at[m, 2, d], to(m, self.second, d))

        def last(self, m):
            return remote(m, self.base + 6, self.by.at[m, 2, 1 - z], self.bz.at[m], to(m, "z", 0))

        def S_far(self, m):
            slot, p = lax.rem(m, 2), self.at(m)[0]
            for d in range(2):
                for q in range(4):
                    self.stage[slot, 0, d, q] = self.own(m, lax.rem(p + 2, 4), q, d)
                self.far1(m, d).start()

        def S_own(self, m):
            slot, p = lax.rem(m, 2), self.at(m)[0]
            for d in range(2):
                for q in range(4):
                    self.stage[slot, 1, d, q] = self.own(m, step_of(p, d), q, 1 - d)
                self.own1(m, d).start()

        def A1(self, m):
            p = self.at(m)[0]
            for d in range(2):
                self.far1(m, d).wait_recv()
                for q in range(4):
                    self.bx[m, 0, d, q] += self.own(m, step_of(p, d), q, d)
                self.acc1(m, d).start()

        def F1(self, m):
            p = self.at(m)[0]
            arrived(m, self.base + 2, self.bx.at[m, pl.ds(1, 2)])
            for h in range(2):
                for q in range(4):
                    self.bx[m, 2, h, q] += self.own(m, p, q, h) + self.bx[m, 1, 1 - h, q]
            for d in range(2):
                self.far2(m, d).start()
            for d in range(2):
                self.own2(m, d).start()

        def A2(self, m):
            q = self.at(m)[1]
            for d in range(2):
                self.far2(m, d).wait_recv()
                self.by[m, 0, d] += self.bx[m, 2, d, step_of(q, d)]
                self.acc2(m, d).start()

        def F2(self, m):
            q = self.at(m)[1]
            arrived(m, self.base + 5, self.by.at[m, pl.ds(1, 2)])
            for h in range(2):
                self.by[m, 2, h] += self.bx[m, 2, h, q] + self.by[m, 1, 1 - h]
            self.last(m).start()

        def arrive(self, m):
            self.last(m).wait_recv()

        def total(self, m, rows):
            return self.by[m, 2, z, rows] + self.bz[m, rows]

        def staged(self, m):
            left(m, self.stage.at[lax.rem(m, 2)], self.kind)

    class ZFirst:
        def us(self, m, j):
            return lax.rem(place(m)[0] + (2, 1, 3, 0)[j], 4)

        def zsend(self, m, j):
            return remote(m, 14 + j, S2.at[lax.rem(m, 2), self.us(m, j)], Z2.at[m, self.us(m, j)],
                          to(m, "z", 0), 2)

        def far1(self, m, d):
            return remote(m, 18 + d, Z2.at[m, self.us(m, 0), pl.ds(2 * d, 2)],
                          X2.at[m, 0, pl.ds(2 * d, 2)], to(m, "u", d))

        def own1(self, m, d):
            return remote(m, 20, Z2.at[m, self.us(m, 1 + d), pl.ds(2 - 2 * d, 2)],
                          X2.at[m, 1, pl.ds(2 - 2 * d, 2)], to(m, "u", d))

        def acc1(self, m, d):
            return remote(m, 20, X2.at[m, 0, pl.ds(2 * d, 2)], X2.at[m, 2, pl.ds(2 * d, 2)],
                          to(m, "u", d))

        def far2(self, m, d):
            part = pl.ds(*PARTS[d])
            return remote(m, 21 + d, X2.at[m, 2, lax.rem(place(m)[1] + 2, 4), part],
                          Y2.at[m, 0, part], to(m, "v", d))

        def own2(self, m, d):
            part = pl.ds(*PARTS[1 - d])
            return remote(m, 23, X2.at[m, 2, step_of(place(m)[1], d), part],
                          Y2.at[m, 1, part], to(m, "v", d))

        def acc2(self, m, d):
            part = pl.ds(*PARTS[d])
            return remote(m, 23, Y2.at[m, 0, part], Y2.at[m, 2, part], to(m, "v", d))

        def S(self, m, js):
            slot = lax.rem(m, 2)
            for j in js:
                for v in range(4):
                    S2[slot, self.us(m, j), v] = local(2, m, self.us(m, j), v, 1 - z)
                self.zsend(m, j).start()

        def Z(self, m, j):
            self.zsend(m, j).wait_recv()
            for v in range(4):
                Z2[m, self.us(m, j), v] += local(2, m, self.us(m, j), v, z)

        def Z1a(self, m):
            self.Z(m, 0)
            for d in range(2):
                self.far1(m, d).start()
            self.Z(m, 1)
            self.own1(m, 0).start()

        def Z1b(self, m):
            self.Z(m, 2)
            self.own1(m, 1).start()
            self.Z(m, 3)

        def A1(self, m):
            for d in range(2):
                self.far1(m, d).wait_recv()
                for i in range(2):
                    X2[m, 0, 2 * d + i] += Z2[m, self.us(m, 1 + d), 2 * d + i]
                self.acc1(m, d).start()

        def F1(self, m):
            arrived(m, 20, X2.at[m, pl.ds(1, 2)])
            for v in range(4):
                X2[m, 2, v] += Z2[m, place(m)[0], v] + X2[m, 1, v]
            for d in range(2):
                self.far2(m, d).start()
            for d in range(2):
                self.own2(m, d).start()

        def A2(self, m):
            for d in range(2):
                self.far2(m, d).wait_recv()
                part = pl.ds(*PARTS[d])
                Y2[m, 0, part] += X2[m, 2, step_of(place(m)[1], d), part]
                self.acc2(m, d).start()

        def arrive(self, m):
            arrived(m, 23, Y2.at[m, pl.ds(1, 2)])

        def total(self, m, rows):
            return X2[m, 2, place(m)[1], rows] + Y2[m, 1, rows] + Y2[m, 2, rows]

        def staged(self, m):
            left(m, S2.at[lax.rem(m, 2)], 2)

    A = Plane(0, "u", "v", S0, X0, Y0, Z0)
    B = Plane(1, "v", "u", S1b, X1, Y1, Z1)
    C = ZFirst()

    def begin(m):
        @pl.when(m >= 2)
        def _():
            for color in (A, B, C):
                color.staged(m - 2)

        load_g(m, 0).wait()
        B.S_far(m)
        load_g(m, 1).wait()
        A.S_far(m)
        load_g(m, 2).wait()
        C.S(m, (0,))

        @pl.when(m + 2 < N)
        def _():
            for i in range(3):
                load_g(m + 2, i).start()

        B.S_own(m)
        A.S_own(m)
        C.S(m, (1, 2, 3))
        for c in load_state(m):
            c.wait()

        @pl.when(m == 0)
        def _():
            for c in scalars:
                c.wait()

        @pl.when(m + 1 < N)
        def _():
            for c in load_state(m + 1):
                c.start()

    def update(m, color, r0, size):
        color.arrive(m)
        t, g = lax.div(m, 2), lax.rem(m, 2)
        scale, top = ms_ref[t], vm_ref[g, t]
        inverse = 1.0 / jnp.full((8, LANES), ve_ref[g, t], jnp.float32)[0:1]
        hi = peak = jnp.zeros((8, LANES), jnp.float32)
        lo = hi + 3e38
        at = r0
        while at < r0 + size:
            base = at // 16 * 16
            rows = min(base + 32 if base == at else base + 16, r0 + size) - at
            here = pl.ds(at, rows)
            half = lambda ref: ref[m, base : base + 32 if rows > 16 else base + 16].astype(
                jnp.float32
            )[at - base : at - base + rows]
            gr = color.total(m, pl.ds(at - r0, rows)) * (1.0 / 32)
            m_old = scale * half(qm)
            v_old = top * jnp.exp(jnp.log(half(qv)) * inverse)
            m_new = 0.9 * m_old + 0.1 * gr
            v_new = 0.95 * v_old + 0.05 * gr * gr
            w = par[m, here]
            par[m, here] = w - 0.02 * (m_new / (jnp.sqrt(v_new) + 1e-8) + 0.1 * w)
            mnew[m, here] = m_new
            lv[m, here] = jnp.log(v_new)
            fold = lambda v: v.reshape(rows // 8, 8, LANES)
            hi = jnp.maximum(hi, jnp.max(fold(v_new), axis=0))
            lo = jnp.minimum(lo, jnp.min(fold(v_new), axis=0))
            peak = jnp.maximum(peak, jnp.max(fold(jnp.abs(m_new)), axis=0))
            at += rows
        row = stat[0:1]
        for i, v in enumerate((hi, -lo, peak)):
            v = jnp.max(jnp.max(v, axis=0, keepdims=True), axis=1, keepdims=True)
            row = jnp.where(lane == 8 * i + 4 * g + t, jnp.maximum(row, v), row)
        stat[0:1] = row

    def drain(m):
        left(m, G.at[m, :, :, :, pl.ds(0, 240)])

    def update_c(m):
        pl.when(m >= 1)(lambda: drain(m - 1))
        update(m, C, 168, 88)

    stat[...] = jnp.full(stat.shape, -3e38, jnp.float32)
    ops = dict(S1=begin, A1y=B.A1, A1x=A.A1, Z1a=C.Z1a, Z1b=C.Z1b, F1y=B.F1, F1x=A.F1,
               A2z=C.A1, A2y=B.A2, A2x=A.A2, F2z=C.F1, F2y=B.F2, F2x=A.F2, A3z=C.A2,
               EA=lambda m: update(m, A, 0, 64), EB=lambda m: update(m, B, 64, 104), EC=update_c)
    assert all(LAGS["EC"] + 1 > v for v in LAGS.values())

    flip = lambda v, b: v + b - 2 * b * v
    plane_peers = [
        {"y": lax.rem(y + j, 4), "x": lax.rem(x + k, 4)}
        for j in (2, 1, 3, 0) for k in (2, 1, 3, 0) if j or k
    ]
    column_peers = [
        {"zl": flip(z, i & 1), "core": flip(core, i >> 1 & 1), "zh": flip(zh, i >> 2)}
        for i in range(1, 8)
    ]

    for i in range(3):
        load_g(0, i).start()
    barrier = pltpu.get_barrier_semaphore()
    peers = [to(0, axis, d) for axis in ("u", "v") for d in range(2)]
    peers += [p for i, p in enumerate(column_peers, 1) if i not in (4, 6)]
    for peer in peers:
        pl.semaphore_signal(barrier, inc=1, device_id=peer, device_id_type=MESH)
    pl.semaphore_wait(barrier, len(peers))
    for i in range(3):
        load_g(1, i).start()
    for c in load_state(0) + scalars:
        c.start()

    def step(k, _):
        for name in ORDER:
            m = k - LAGS[name]
            pl.when((m >= 0) & (m < N))(lambda f=ops[name], m=m: f(m))
        return 0

    lax.fori_loop(0, N + max(LAGS.values()), step, 0)

    for phase, (who, buf) in enumerate(((plane_peers, wide), (column_peers, deep))):
        copies = [
            pltpu.make_async_remote_copy(
                src_ref=stat.at[pl.ds(8 * phase, 1)], dst_ref=buf.at[pl.ds(i, 1)],
                send_sem=atsem.at[phase], recv_sem=asem.at[phase],
                device_id=peer, device_id_type=MESH,
            )
            for i, peer in enumerate(who)
        ]
        for c in copies:
            c.start()
        mine = stat[8 * phase : 8 * phase + 1]
        buf[len(who) : len(who) + 1] = mine
        if phase == 0:
            drain(N - 1)
            for m in (N - 2, N - 1):
                for color in (A, B, C):
                    color.staged(m)
        everyone = pltpu.make_async_remote_copy(
            src_ref=buf.at[pl.ds(0, len(who))], dst_ref=buf.at[pl.ds(0, len(who))],
            send_sem=atsem.at[phase], recv_sem=asem.at[phase],
            device_id=who[0], device_id_type=MESH,
        )
        everyone.wait_recv()
        most = jnp.max(buf[...], axis=0, keepdims=True)
        if phase == 0:
            stat[8:9] = most
        else:
            table[...] = jnp.where(lane < 16, jnp.maximum(mine, buf[0:1]), most)
        everyone.wait_send()


def finish(par, mnew, lv, table, np_hbm, nqm_hbm, nms_ref, nqv_hbm, nvm_ref, nve_ref, qmo, qvo, sem):
    def store_out(m, i):
        h, v = ((np_hbm, par), (nqm_hbm, qmo), (nqv_hbm, qvo))[i]
        return pltpu.make_async_copy(v.at[m], columns(h, m), sem.at[m, i])

    for m in range(N):
        store_out(m, 0).start()
    row = table[...]
    lane = lax.broadcasted_iota(jnp.int32, (1, LANES), 1)
    left = lambda v, k: pltpu.roll(v, LANES - k, 1)
    low, peak = -left(row, 8), left(row, 16)
    scale = jnp.maximum(peak, left(peak, 4)) + 1e-6
    new_exp = 12.343 / jnp.maximum(jnp.log(row / low), 1.0)
    log_top, inverse = jnp.log(row), 1.0 / scale
    pick = lambda v, i: jnp.max(jnp.where(lane == i, v, -3e38), axis=1, keepdims=True)
    for m in range(N):
        t, g = m // 2, m % 2
        qmo[m] = (mnew[m] * pick(inverse, t)).astype(jnp.bfloat16)
        store_out(m, 1).start()
        e, top = pick(new_exp, 4 * g + t), pick(log_top, 4 * g + t)
        qvo[m] = jnp.exp(e * (lv[m] - top)).astype(jnp.bfloat16)
        store_out(m, 2).start()
    nms_ref[...] = scale[:, 0:4]
    for g in range(2):
        nvm_ref[g : g + 1, :] = left(row, 4 * g)[:, 0:4] if g else row[:, 0:4]
        nve_ref[g : g + 1, :] = left(new_exp, 4 * g)[:, 0:4] if g else new_exp[:, 0:4]
    for m in range(N):
        for i in range(3):
            store_out(m, i).wait()


def on_device(grads, param, q_m, m_scale, q_v, v_max, v_exp):
    f32, bf16 = jnp.float32, jnp.bfloat16
    a, b, c = SPLIT
    plane = lambda s: [
        pltpu.VMEM((2, 2, 2, 4, s, LANES), f32),
        pltpu.VMEM((N, 3, 2, 4, s, LANES), f32),
        pltpu.VMEM((N, 3, 2, s, LANES), f32),
        pltpu.VMEM((N, s, LANES), f32),
    ]
    block = lambda kind: pltpu.VMEM((N, ROWS, LANES), kind)
    anywhere = pl.BlockSpec(memory_space=pl.ANY)
    vmem = pl.BlockSpec(memory_space=pltpu.VMEM)
    kept = pl.pallas_call(
        kernel,
        out_shape=(block(f32), block(f32), block(f32), pltpu.VMEM((1, LANES), f32)),
        in_specs=[anywhere] * 7,
        out_specs=(vmem,) * 4,
        scratch_shapes=[
            pltpu.VMEM((N, 4, 4, 2, ROWS, LANES), bf16),
            *plane(a),
            *plane(b),
            pltpu.VMEM((2, 4, 4, c, LANES), f32),
            pltpu.VMEM((N, 4, 4, c, LANES), f32),
            pltpu.VMEM((N, 3, 4, c, LANES), f32),
            pltpu.VMEM((N, 3, c, LANES), f32),
            block(bf16), block(bf16),
            pltpu.VMEM((16, LANES), f32),
            pltpu.VMEM((16, LANES), f32),
            pltpu.VMEM((8, LANES), f32),
            pltpu.SMEM((4,), f32),
            pltpu.SMEM((2, 4), f32),
            pltpu.SMEM((2, 4), f32),
            pltpu.SemaphoreType.DMA((N, SEMS)),
            pltpu.SemaphoreType.DMA((N,)),
            pltpu.SemaphoreType.DMA((2, 3)),
            pltpu.SemaphoreType.DMA((2, 3)),
            pltpu.SemaphoreType.DMA((3,)),
            pltpu.SemaphoreType.DMA((2,)),
            pltpu.SemaphoreType.DMA((2,)),
            pltpu.SemaphoreType.DMA((3,)),
        ],
        compiler_params=pltpu.CompilerParams(
            collective_id=0, has_side_effects=True, vmem_limit_bytes=LIMIT
        ),
    )(grads[0].reshape(4, 4, 4, 2, ROWS, 2 * LANES), param, q_m, m_scale, q_v, v_max.T, v_exp.T)
    small = lambda rows: jax.ShapeDtypeStruct((rows, 4), f32)
    new_param, new_q_m, ms, new_q_v, vm, ve = pl.pallas_call(
        finish,
        out_shape=(
            jax.ShapeDtypeStruct(param.shape, f32),
            jax.ShapeDtypeStruct(q_m.shape, bf16),
            small(1),
            jax.ShapeDtypeStruct(q_v.shape, bf16),
            small(2),
            small(2),
        ),
        in_specs=[vmem] * 4,
        out_specs=(anywhere, anywhere, vmem, anywhere, vmem, vmem),
        scratch_shapes=[block(bf16), block(bf16), pltpu.SemaphoreType.DMA((N, 3))],
        compiler_params=pltpu.CompilerParams(vmem_limit_bytes=8 * 2**20),
    )(*kept)
    return new_param, new_q_m, ms[0], new_q_v, vm.T, ve.T


def solution(mesh):
    split = Mesh(mesh.devices.reshape(2, 2, 4, 4, 2), TENSOR + DP)
    return jax.shard_map(
        on_device,
        mesh=split,
        in_specs=(
            P(DP, None, None, TENSOR),
            P(None, DP, TENSOR),
            P(None, DP, TENSOR),
            P(),
            P(None, DP, TENSOR),
            P(None, TENSOR),
            P(None, TENSOR),
        ),
        out_specs=(
            P(None, DP, TENSOR),
            P(None, DP, TENSOR),
            P(),
            P(None, DP, TENSOR),
            P(None, TENSOR),
            P(None, TENSOR),
        ),
        check_vma=False,
    )
```

```python
import jax
import jax.numpy as jnp
from jax import lax
from jax.experimental import pallas as pl
from jax.experimental.pallas import tpu as pltpu
from jax.sharding import Mesh
from jax.sharding import PartitionSpec as P

MESH = pl.DeviceIdType.MESH
DP = ("y", "x", "zl")
TENSOR = ("zh", "core")
ROWS = 256
LANES = 128
SPLIT = (64, 104, 88)
PARTS = ((0, 48), (48, 40))
LOADS = ((64, 112), (0, 64), (176, 80))
N = 8
SEMS = 16
LIMIT = 55 * 2**20
ORDER = ('A1y', 'A2z', 'F2y', 'F2x', 'EC', 'EA', 'A1x', 'A3z', 'F2z', 'F1y', 'A2x', 'A2y', 'Z1a', 'F1x', 'Z1b', 'EB', 'S1')
LAGS = {'S1': 0, 'A1y': 2, 'A1x': 2, 'Z1a': 3, 'Z1b': 4, 'F1y': 3, 'F1x': 3, 'A2z': 7, 'A2y': 4, 'A2x': 8, 'F2z': 20, 'F2y': 8, 'F2x': 22, 'A3z': 34, 'EA': 36, 'EB': 22, 'EC': 51}


def columns(ref, m):
    t, g = lax.div(m, 2), lax.rem(m, 2)
    return ref.at[t, ..., pl.ds(pl.multiple_of(g * LANES, LANES), LANES)]


def kernel(
    g_hbm, p_hbm, qm_hbm, ms_hbm, qv_hbm, vm_hbm, ve_hbm,
    par, mnew, lv, table,
    G, S0, X0, Y0, Z0, S1b, X1, Y1, Z1, S2, Z2, X2, Y2,
    qm, qv, most, stat, wide, deep, ms_ref, vm_ref, ve_ref,
    rsem, ssem, stsem, gsem, psem, asem, atsem, csem,
):
    y, x, z = lax.axis_index("y"), lax.axis_index("x"), lax.axis_index("zl")
    zh, core = lax.axis_index("zh"), lax.axis_index("core")

    def step_of(coord, d):
        return lax.rem(coord + (1 if d == 0 else 3), 4)

    def place(m):
        s = lax.rem(m, 2)
        return x + s * (y - x), y + s * (x - y)

    def to(m, axis, d):
        if axis == "z":
            return {"zl": 1 - z}
        s = lax.rem(m, 2)
        s = s if axis == "u" else 1 - s
        return {"x": x + (1 - s) * (step_of(x, d) - x), "y": y + s * (step_of(y, d) - y)}

    def remote(m, idx, src, dst, target, staged=None):
        sent = ssem.at[m] if staged is None else stsem.at[lax.rem(m, 2), staged]
        return pltpu.make_async_remote_copy(
            src_ref=src, dst_ref=dst, send_sem=sent, recv_sem=rsem.at[m, idx],
            device_id=target, device_id_type=MESH,
        )

    def arrived(m, idx, block):
        remote(m, idx, block, block, to(m, "u", 0)).wait_recv()

    def left(m, block, staged=None):
        remote(m, 0, block, block, to(m, "u", 0), staged).wait_send()

    def load_g(m, i):
        rows = pl.ds(*LOADS[i])
        return pltpu.make_async_copy(
            columns(g_hbm, m).at[:, :, :, rows], G.at[m, :, :, :, rows], gsem.at[lax.rem(m, 2), i]
        )

    scalars = [
        pltpu.make_async_copy(h, v, csem.at[i])
        for i, (h, v) in enumerate(((ms_hbm, ms_ref), (vm_hbm, vm_ref), (ve_hbm, ve_ref)))
    ]

    def load_state(m):
        return [
            pltpu.make_async_copy(columns(h, m), v.at[m], psem.at[i])
            for i, (h, v) in enumerate(((p_hbm, par), (qm_hbm, qm), (qv_hbm, qv)))
        ]

    def local(kind, m, uu, vv, zz):
        s = lax.rem(m, 2)
        yy, xx = vv + s * (uu - vv), uu + s * (vv - uu)
        if kind == 0:
            return G[m, yy, xx, zz, 0:64, :].astype(jnp.float32)
        if kind == 1:
            return G[m, yy, xx, zz, 64:176, :].astype(jnp.float32)[:104]
        return G[m, yy, xx, zz, 160:256, :].astype(jnp.float32)[8:]

    class Plane:
        def __init__(self, kind, first, second, stage, bx, by, bz):
            self.kind, self.first, self.second = kind, first, second
            self.stage, self.bx, self.by, self.bz, self.base = stage, bx, by, bz, 5 * kind

        def own(self, m, pp, qq, zz):
            uu, vv = (pp, qq) if self.first == "u" else (qq, pp)
            return local(self.kind, m, uu, vv, zz)

        def at(self, m):
            u, v = place(m)
            return (u, v) if self.first == "u" else (v, u)

        def far1(self, m, d):
            return remote(m, self.base, self.stage.at[lax.rem(m, 2), 0, d],
                          self.bx.at[m, 0, d], to(m, self.first, d), self.kind)

        def own1(self, m, d):
            return remote(m, self.base + 1, self.stage.at[lax.rem(m, 2), 1, d],
                          self.bx.at[m, 1, d], to(m, self.first, d), self.kind)

        def acc1(self, m, d):
            return remote(m, self.base + 1, self.bx.at[m, 0, d],
                          self.bx.at[m, 2, d], to(m, self.first, d))

        def far2(self, m, d):
            q = self.at(m)[1]
            return remote(m, self.base + 2, self.bx.at[m, 2, d, lax.rem(q + 2, 4)],
                          self.by.at[m, 0, d], to(m, self.second, d))

        def own2(self, m, d):
            q = self.at(m)[1]
            return remote(m, self.base + 3, self.bx.at[m, 2, 1 - d, step_of(q, d)],
                          self.by.at[m, 1, d], to(m, self.second, d))

        def acc2(self, m, d):
            return remote(m, self.base + 3, self.by.at[m, 0, d],
                          self.by.at[m, 2, d], to(m, self.second, d))

        def last(self, m):
            return remote(m, self.base + 4, self.by.at[m, 2, 1 - z], self.bz.at[m], to(m, "z", 0))

        def S_far(self, m):
            slot, p = lax.rem(m, 2), self.at(m)[0]
            for d in range(2):
                for q in range(4):
                    self.stage[slot, 0, d, q] = self.own(m, lax.rem(p + 2, 4), q, d)
                self.far1(m, d).start()

        def S_own(self, m):
            slot, p = lax.rem(m, 2), self.at(m)[0]
            for d in range(2):
                for q in range(4):
                    self.stage[slot, 1, d, q] = self.own(m, step_of(p, d), q, 1 - d)
                self.own1(m, d).start()

        def A1(self, m):
            p = self.at(m)[0]
            arrived(m, self.base, self.bx.at[m, 0])
            for d in range(2):
                for q in range(4):
                    self.bx[m, 0, d, q] += self.own(m, step_of(p, d), q, d)
                self.acc1(m, d).start()

        def F1(self, m):
            p = self.at(m)[0]
            arrived(m, self.base + 1, self.bx.at[m, pl.ds(1, 2)])
            for h in range(2):
                for q in range(4):
                    self.bx[m, 2, h, q] += self.own(m, p, q, h) + self.bx[m, 1, 1 - h, q]
            for d in range(2):
                self.far2(m, d).start()
            for d in range(2):
                self.own2(m, d).start()

        def A2(self, m):
            q = self.at(m)[1]
            arrived(m, self.base + 2, self.by.at[m, 0])
            for d in range(2):
                self.by[m, 0, d] += self.bx[m, 2, d, step_of(q, d)]
                self.acc2(m, d).start()

        def F2(self, m):
            q = self.at(m)[1]
            arrived(m, self.base + 3, self.by.at[m, pl.ds(1, 2)])
            for h in range(2):
                self.by[m, 2, h] += self.bx[m, 2, h, q] + self.by[m, 1, 1 - h]
            self.last(m).start()

        def arrive(self, m):
            self.last(m).wait_recv()

        def total(self, m, rows):
            return self.by[m, 2, z, rows] + self.bz[m, rows]

        def staged(self, m):
            left(m, self.stage.at[lax.rem(m, 2)], self.kind)

    class ZFirst:
        def us(self, m, j):
            return lax.rem(place(m)[0] + (2, 1, 3, 0)[j], 4)

        def zsend(self, m, j):
            return remote(m, 10 + j // 2, S2.at[lax.rem(m, 2), self.us(m, j)], Z2.at[m, self.us(m, j)],
                          to(m, "z", 0), 2)

        def far1(self, m, d):
            return remote(m, 12, Z2.at[m, self.us(m, 0), pl.ds(2 * d, 2)],
                          X2.at[m, 0, pl.ds(2 * d, 2)], to(m, "u", d))

        def own1(self, m, d):
            return remote(m, 13, Z2.at[m, self.us(m, 1 + d), pl.ds(2 - 2 * d, 2)],
                          X2.at[m, 1, pl.ds(2 - 2 * d, 2)], to(m, "u", d))

        def acc1(self, m, d):
            return remote(m, 13, X2.at[m, 0, pl.ds(2 * d, 2)], X2.at[m, 2, pl.ds(2 * d, 2)],
                          to(m, "u", d))

        def far2(self, m, d):
            part = pl.ds(*PARTS[d])
            return remote(m, 14, X2.at[m, 2, lax.rem(place(m)[1] + 2, 4), part],
                          Y2.at[m, 0, part], to(m, "v", d))

        def own2(self, m, d):
            part = pl.ds(*PARTS[1 - d])
            return remote(m, 15, X2.at[m, 2, step_of(place(m)[1], d), part],
                          Y2.at[m, 1, part], to(m, "v", d))

        def acc2(self, m, d):
            part = pl.ds(*PARTS[d])
            return remote(m, 15, Y2.at[m, 0, part], Y2.at[m, 2, part], to(m, "v", d))

        def S(self, m, js):
            slot = lax.rem(m, 2)
            for j in js:
                for v in range(4):
                    S2[slot, self.us(m, j), v] = local(2, m, self.us(m, j), v, 1 - z)
                self.zsend(m, j).start()

        def Z(self, m, j):
            for v in range(4):
                Z2[m, self.us(m, j), v] += local(2, m, self.us(m, j), v, z)

        def Z1a(self, m):
            arrived(m, 10, Z2.at[m, pl.ds(0, 2)])
            self.Z(m, 0)
            for d in range(2):
                self.far1(m, d).start()
            self.Z(m, 1)
            self.own1(m, 0).start()

        def Z1b(self, m):
            arrived(m, 11, Z2.at[m, pl.ds(0, 2)])
            self.Z(m, 2)
            self.own1(m, 1).start()
            self.Z(m, 3)

        def A1(self, m):
            arrived(m, 12, X2.at[m, 0])
            for d in range(2):
                for i in range(2):
                    X2[m, 0, 2 * d + i] += Z2[m, self.us(m, 1 + d), 2 * d + i]
                self.acc1(m, d).start()

        def F1(self, m):
            arrived(m, 13, X2.at[m, pl.ds(1, 2)])
            for v in range(4):
                X2[m, 2, v] += Z2[m, place(m)[0], v] + X2[m, 1, v]
            for d in range(2):
                self.far2(m, d).start()
            for d in range(2):
                self.own2(m, d).start()

        def A2(self, m):
            arrived(m, 14, Y2.at[m, 0])
            for d in range(2):
                part = pl.ds(*PARTS[d])
                Y2[m, 0, part] += X2[m, 2, step_of(place(m)[1], d), part]
                self.acc2(m, d).start()

        def arrive(self, m):
            arrived(m, 15, Y2.at[m, pl.ds(1, 2)])

        def total(self, m, rows):
            return X2[m, 2, place(m)[1], rows] + Y2[m, 1, rows] + Y2[m, 2, rows]

        def staged(self, m):
            left(m, S2.at[lax.rem(m, 2)], 2)

    A = Plane(0, "u", "v", S0, X0, Y0, Z0)
    B = Plane(1, "v", "u", S1b, X1, Y1, Z1)
    C = ZFirst()

    def begin(m):
        @pl.when(m >= 2)
        def _():
            for color in (A, B, C):
                color.staged(m - 2)

        load_g(m, 0).wait()
        B.S_far(m)
        load_g(m, 1).wait()
        A.S_far(m)
        load_g(m, 2).wait()
        C.S(m, (0,))

        @pl.when(m + 2 < N)
        def _():
            for i in range(3):
                load_g(m + 2, i).start()

        B.S_own(m)
        A.S_own(m)
        C.S(m, (1, 2, 3))
        for c in load_state(m):
            c.wait()

        @pl.when(m == 0)
        def _():
            for c in scalars:
                c.wait()

        @pl.when(m + 1 < N)
        def _():
            for c in load_state(m + 1):
                c.start()

    def update(m, color, r0, size):
        color.arrive(m)
        t, g = lax.div(m, 2), lax.rem(m, 2)
        scale, top = ms_ref[t], vm_ref[g, t]
        inverse = 1.0 / jnp.full((8, LANES), ve_ref[g, t], jnp.float32)[0:1]
        hi = peak = jnp.zeros((8, LANES), jnp.float32)
        lo = hi + 3e38
        at = r0
        while at < r0 + size:
            base = at // 16 * 16
            rows = min(base + 32 if base == at else base + 16, r0 + size) - at
            here = pl.ds(at, rows)
            half = lambda ref: ref[m, base : base + 32 if rows > 16 else base + 16].astype(
                jnp.float32
            )[at - base : at - base + rows]
            gr = color.total(m, pl.ds(at - r0, rows)) * (1.0 / 32)
            m_old = scale * half(qm)
            v_old = top * jnp.exp(jnp.log(half(qv)) * inverse)
            m_new = 0.9 * m_old + 0.1 * gr
            v_new = 0.95 * v_old + 0.05 * gr * gr
            w = par[m, here]
            par[m, here] = w - 0.02 * (m_new / (jnp.sqrt(v_new) + 1e-8) + 0.1 * w)
            mnew[m, here] = m_new
            lv[m, here] = jnp.log(v_new)
            fold = lambda v: v.reshape(rows // 8, 8, LANES)
            hi = jnp.maximum(hi, jnp.max(fold(v_new), axis=0))
            lo = jnp.minimum(lo, jnp.min(fold(v_new), axis=0))
            peak = jnp.maximum(peak, jnp.max(fold(jnp.abs(m_new)), axis=0))
            at += rows
        for i, v in enumerate((hi, -lo, peak)):
            most[i, m] = jnp.maximum(most[i, m], v)

    def drain(m):
        left(m, G.at[m, :, :, :, pl.ds(0, 240)])

    def update_c(m):
        pl.when(m >= 1)(lambda: drain(m - 1))
        update(m, C, 168, 88)

    most[...] = jnp.full(most.shape, -3e38, jnp.float32)
    ops = dict(S1=begin, A1y=B.A1, A1x=A.A1, Z1a=C.Z1a, Z1b=C.Z1b, F1y=B.F1, F1x=A.F1,
               A2z=C.A1, A2y=B.A2, A2x=A.A2, F2z=C.F1, F2y=B.F2, F2x=A.F2, A3z=C.A2,
               EA=lambda m: update(m, A, 0, 64), EB=lambda m: update(m, B, 64, 104), EC=update_c)
    assert all(LAGS["EC"] + 1 > v for v in LAGS.values())

    flip = lambda v, b: v + b - 2 * b * v
    plane_peers = [
        {"y": lax.rem(y + j, 4), "x": lax.rem(x + k, 4)}
        for j in (2, 1, 3, 0) for k in (2, 1, 3, 0) if j or k
    ]
    column_peers = [
        {"zl": flip(z, i & 1), "core": flip(core, i >> 1 & 1), "zh": flip(zh, i >> 2)}
        for i in range(7, 0, -1)
    ]

    for i in range(3):
        load_g(0, i).start()
    barrier = pltpu.get_barrier_semaphore()
    peers = [to(0, axis, d) for axis in ("u", "v") for d in range(2)]
    peers += [p for i, p in enumerate(column_peers) if i not in (1, 3)]
    for peer in peers:
        pl.semaphore_signal(barrier, inc=1, device_id=peer, device_id_type=MESH)
    pl.semaphore_wait(barrier, len(peers))
    for i in range(3):
        load_g(1, i).start()
    for c in load_state(0) + scalars:
        c.start()

    def step(k, _):
        for name in ORDER:
            m = k - LAGS[name]
            pl.when((m >= 0) & (m < N))(lambda f=ops[name], m=m: f(m))
        return 0

    lax.fori_loop(0, N + max(LAGS.values()), step, 0)

    sub = lax.broadcasted_iota(jnp.int32, (N, LANES), 0)
    lane = lax.broadcasted_iota(jnp.int32, (N, LANES), 1)
    spread = jnp.full((N, LANES), -3e38, jnp.float32)
    for i in range(3):
        v = jnp.max(jnp.max(most[i], axis=1), axis=1, keepdims=True)
        spread = jnp.where(lane == 8 * i + 4 * lax.rem(sub, 2) + lax.div(sub, 2), v, spread)
    stat[0:1] = jnp.max(spread, axis=0, keepdims=True)
    lane = lane[0:1]
    for phase, (who, buf) in enumerate(((plane_peers, wide), (column_peers, deep))):
        copies = [
            pltpu.make_async_remote_copy(
                src_ref=stat.at[pl.ds(8 * phase, 1)], dst_ref=buf.at[pl.ds(i, 1)],
                send_sem=atsem.at[phase], recv_sem=asem.at[phase],
                device_id=peer, device_id_type=MESH,
            )
            for i, peer in enumerate(who)
        ]
        for c in copies:
            c.start()
        mine = stat[8 * phase : 8 * phase + 1]
        buf[len(who) : len(who) + 1] = mine
        if phase == 0:
            drain(N - 1)
            for m in (N - 2, N - 1):
                for color in (A, B, C):
                    color.staged(m)
        everyone = pltpu.make_async_remote_copy(
            src_ref=buf.at[pl.ds(0, len(who))], dst_ref=buf.at[pl.ds(0, len(who))],
            send_sem=atsem.at[phase], recv_sem=asem.at[phase],
            device_id=who[0], device_id_type=MESH,
        )
        everyone.wait_recv()
        top = jnp.max(buf[...], axis=0, keepdims=True)
        if phase == 0:
            stat[8:9] = top
        else:
            table[...] = jnp.where(lane < 16, jnp.maximum(mine, buf[6:7]), top)
        everyone.wait_send()


def finish(par, mnew, lv, table, np_hbm, nqm_hbm, nms_ref, nqv_hbm, nvm_ref, nve_ref, qmo, qvo, sem):
    def store_out(m, i):
        h, v = ((np_hbm, par), (nqm_hbm, qmo), (nqv_hbm, qvo))[i]
        return pltpu.make_async_copy(v.at[m], columns(h, m), sem.at[i])

    for m in range(N):
        store_out(m, 0).start()
    row = table[...]
    lane = lax.broadcasted_iota(jnp.int32, (1, LANES), 1)
    left = lambda v, k: pltpu.roll(v, LANES - k, 1)
    low, peak = -left(row, 8), left(row, 16)
    scale = jnp.maximum(peak, left(peak, 4)) + 1e-6
    new_exp = 12.343 / jnp.maximum(jnp.log(row / low), 1.0)
    log_top, inverse = jnp.log(row), 1.0 / scale
    pick = lambda v, i: jnp.max(jnp.where(lane == i, v, -3e38), axis=1, keepdims=True)
    for m in range(N):
        t, g = m // 2, m % 2
        qmo[m] = (mnew[m] * pick(inverse, t)).astype(jnp.bfloat16)
        store_out(m, 1).start()
        e, top = pick(new_exp, 4 * g + t), pick(log_top, 4 * g + t)
        qvo[m] = jnp.exp(e * (lv[m] - top)).astype(jnp.bfloat16)
        store_out(m, 2).start()
    nms_ref[...] = scale[:, 0:4]
    for g in range(2):
        nvm_ref[g : g + 1, :] = left(row, 4 * g)[:, 0:4] if g else row[:, 0:4]
        nve_ref[g : g + 1, :] = left(new_exp, 4 * g)[:, 0:4] if g else new_exp[:, 0:4]
    for i, h in enumerate((np_hbm, nqm_hbm, nqv_hbm)):
        pltpu.make_async_copy(h, h, sem.at[i]).wait()


def on_device(grads, param, q_m, m_scale, q_v, v_max, v_exp):
    f32, bf16 = jnp.float32, jnp.bfloat16
    a, b, c = SPLIT
    plane = lambda s: [
        pltpu.VMEM((2, 2, 2, 4, s, LANES), f32),
        pltpu.VMEM((N, 3, 2, 4, s, LANES), f32),
        pltpu.VMEM((N, 3, 2, s, LANES), f32),
        pltpu.VMEM((N, s, LANES), f32),
    ]
    block = lambda kind: pltpu.VMEM((N, ROWS, LANES), kind)
    anywhere = pl.BlockSpec(memory_space=pl.ANY)
    vmem = pl.BlockSpec(memory_space=pltpu.VMEM)
    kept = pl.pallas_call(
        kernel,
        out_shape=(block(f32), block(f32), block(f32), pltpu.VMEM((1, LANES), f32)),
        in_specs=[anywhere] * 7,
        out_specs=(vmem,) * 4,
        scratch_shapes=[
            pltpu.VMEM((N, 4, 4, 2, ROWS, LANES), bf16),
            *plane(a),
            *plane(b),
            pltpu.VMEM((2, 4, 4, c, LANES), f32),
            pltpu.VMEM((N, 4, 4, c, LANES), f32),
            pltpu.VMEM((N, 3, 4, c, LANES), f32),
            pltpu.VMEM((N, 3, c, LANES), f32),
            block(bf16), block(bf16),
            pltpu.VMEM((3, N, 8, LANES), f32),
            pltpu.VMEM((16, LANES), f32),
            pltpu.VMEM((16, LANES), f32),
            pltpu.VMEM((8, LANES), f32),
            pltpu.SMEM((4,), f32),
            pltpu.SMEM((2, 4), f32),
            pltpu.SMEM((2, 4), f32),
            pltpu.SemaphoreType.DMA((N, SEMS)),
            pltpu.SemaphoreType.DMA((N,)),
            pltpu.SemaphoreType.DMA((2, 3)),
            pltpu.SemaphoreType.DMA((2, 3)),
            pltpu.SemaphoreType.DMA((3,)),
            pltpu.SemaphoreType.DMA((2,)),
            pltpu.SemaphoreType.DMA((2,)),
            pltpu.SemaphoreType.DMA((3,)),
        ],
        compiler_params=pltpu.CompilerParams(
            collective_id=0, has_side_effects=True, vmem_limit_bytes=LIMIT
        ),
    )(grads[0].reshape(4, 4, 4, 2, ROWS, 2 * LANES), param, q_m, m_scale, q_v, v_max.T, v_exp.T)
    small = lambda rows: jax.ShapeDtypeStruct((rows, 4), f32)
    new_param, new_q_m, ms, new_q_v, vm, ve = pl.pallas_call(
        finish,
        out_shape=(
            jax.ShapeDtypeStruct(param.shape, f32),
            jax.ShapeDtypeStruct(q_m.shape, bf16),
            small(1),
            jax.ShapeDtypeStruct(q_v.shape, bf16),
            small(2),
            small(2),
        ),
        in_specs=[vmem] * 4,
        out_specs=(anywhere, anywhere, vmem, anywhere, vmem, vmem),
        scratch_shapes=[block(bf16), block(bf16), pltpu.SemaphoreType.DMA((3,))],
        compiler_params=pltpu.CompilerParams(vmem_limit_bytes=8 * 2**20),
    )(*kept)
    return new_param, new_q_m, ms[0], new_q_v, vm.T, ve.T


def solution(mesh):
    split = Mesh(mesh.devices.reshape(2, 2, 4, 4, 2), TENSOR + DP)
    return jax.shard_map(
        on_device,
        mesh=split,
        in_specs=(
            P(DP, None, None, TENSOR),
            P(None, DP, TENSOR),
            P(None, DP, TENSOR),
            P(),
            P(None, DP, TENSOR),
            P(None, TENSOR),
            P(None, TENSOR),
        ),
        out_specs=(
            P(None, DP, TENSOR),
            P(None, DP, TENSOR),
            P(),
            P(None, DP, TENSOR),
            P(None, TENSOR),
            P(None, TENSOR),
        ),
        check_vma=False,
    )
```

```python
import jax
import jax.numpy as jnp
from jax import lax
from jax.experimental import pallas as pl
from jax.experimental.pallas import tpu as pltpu
from jax.sharding import Mesh
from jax.sharding import PartitionSpec as P

MESH = pl.DeviceIdType.MESH
DP = ("y", "x", "zl")
TENSOR = ("zh", "core")
ROWS = 256
LANES = 128
SPLIT = (64, 104, 88)
PARTS = ((0, 48), (48, 40))
LOADS = ((64, 112), (0, 64), (176, 80))
N = 8
SEMS = 16
LIMIT = 55 * 2**20
ORDER = ('F2x', 'EC', 'A1x', 'EA', 'A1y', 'A2z', 'F2z', 'F1y', 'F2y', 'Z1a', 'A2y', 'F1x', 'A2x', 'A3z', 'EB', 'Z1b', 'S1')
LAGS = {'S1': 0, 'A1y': 2, 'A1x': 2, 'Z1a': 3, 'Z1b': 3, 'F1y': 3, 'F1x': 3, 'A2z': 7, 'A2y': 4, 'A2x': 6, 'F2z': 17, 'F2y': 8, 'F2x': 20, 'A3z': 24, 'EA': 28, 'EB': 20, 'EC': 33}


def columns(ref, m):
    t, g = lax.div(m, 2), lax.rem(m, 2)
    return ref.at[t, ..., pl.ds(pl.multiple_of(g * LANES, LANES), LANES)]


def kernel(
    g_hbm, p_hbm, qm_hbm, ms_hbm, qv_hbm, vm_hbm, ve_hbm,
    par, mnew, lv, table,
    G, S0, X0, Y0, Z0, S1b, X1, Y1, Z1, S2, Z2, X2, Y2,
    qm, qv, most, stat, wide, deep, ms_ref, vm_ref, ve_ref,
    rsem, ssem, stsem, gsem, psem, asem, atsem, csem,
):
    y, x, z = lax.axis_index("y"), lax.axis_index("x"), lax.axis_index("zl")
    zh, core = lax.axis_index("zh"), lax.axis_index("core")

    def step_of(coord, d):
        return lax.rem(coord + (1 if d == 0 else 3), 4)

    def place(m):
        s = lax.rem(m, 2)
        return x + s * (y - x), y + s * (x - y)

    def to(m, axis, d):
        if axis == "z":
            return {"zl": 1 - z}
        s = lax.rem(m, 2)
        s = s if axis == "u" else 1 - s
        return {"x": x + (1 - s) * (step_of(x, d) - x), "y": y + s * (step_of(y, d) - y)}

    def remote(m, idx, src, dst, target, staged=None):
        sent = ssem.at[m] if staged is None else stsem.at[lax.rem(m, 2), staged]
        return pltpu.make_async_remote_copy(
            src_ref=src, dst_ref=dst, send_sem=sent, recv_sem=rsem.at[m, idx],
            device_id=target, device_id_type=MESH,
        )

    def arrived(m, idx, block):
        remote(m, idx, block, block, to(m, "u", 0)).wait_recv()

    def left(m, block, staged=None):
        remote(m, 0, block, block, to(m, "u", 0), staged).wait_send()

    def load_g(m, i):
        rows = pl.ds(*LOADS[i])
        return pltpu.make_async_copy(
            columns(g_hbm, m).at[:, :, :, rows], G.at[m, :, :, :, rows], gsem.at[lax.rem(m, 2), i]
        )

    scalars = [
        pltpu.make_async_copy(h, v, csem.at[i])
        for i, (h, v) in enumerate(((ms_hbm, ms_ref), (vm_hbm, vm_ref), (ve_hbm, ve_ref)))
    ]

    def load_state(m):
        return [
            pltpu.make_async_copy(columns(h, m), v.at[m], psem.at[i])
            for i, (h, v) in enumerate(((p_hbm, par), (qm_hbm, qm), (qv_hbm, qv)))
        ]

    def local(kind, m, uu, vv, zz):
        s = lax.rem(m, 2)
        yy, xx = vv + s * (uu - vv), uu + s * (vv - uu)
        if kind == 0:
            return G[m, yy, xx, zz, 0:64, :].astype(jnp.float32)
        if kind == 1:
            return G[m, yy, xx, zz, 64:176, :].astype(jnp.float32)[:104]
        return G[m, yy, xx, zz, 160:256, :].astype(jnp.float32)[8:]

    class Plane:
        def __init__(self, kind, first, second, stage, bx, by, bz):
            self.kind, self.first, self.second = kind, first, second
            self.stage, self.bx, self.by, self.bz, self.base = stage, bx, by, bz, 5 * kind

        def own(self, m, pp, qq, zz):
            uu, vv = (pp, qq) if self.first == "u" else (qq, pp)
            return local(self.kind, m, uu, vv, zz)

        def at(self, m):
            u, v = place(m)
            return (u, v) if self.first == "u" else (v, u)

        def far1(self, m, d):
            return remote(m, self.base, self.stage.at[lax.rem(m, 2), 0, d],
                          self.bx.at[m, 0, d], to(m, self.first, d), self.kind)

        def own1(self, m, d):
            return remote(m, self.base + 1, self.stage.at[lax.rem(m, 2), 1, d],
                          self.bx.at[m, 1, d], to(m, self.first, d), self.kind)

        def acc1(self, m, d):
            return remote(m, self.base + 1, self.bx.at[m, 0, d],
                          self.bx.at[m, 2, d], to(m, self.first, d))

        def far2(self, m, d):
            q = self.at(m)[1]
            return remote(m, self.base + 2, self.bx.at[m, 2, d, lax.rem(q + 2, 4)],
                          self.by.at[m, 0, d], to(m, self.second, d))

        def own2(self, m, d):
            q = self.at(m)[1]
            return remote(m, self.base + 3, self.bx.at[m, 2, 1 - d, step_of(q, d)],
                          self.by.at[m, 1, d], to(m, self.second, d))

        def acc2(self, m, d):
            return remote(m, self.base + 3, self.by.at[m, 0, d],
                          self.by.at[m, 2, d], to(m, self.second, d))

        def last(self, m):
            return remote(m, self.base + 4, self.by.at[m, 2, 1 - z], self.bz.at[m], to(m, "z", 0))

        def S_far(self, m):
            slot, p = lax.rem(m, 2), self.at(m)[0]
            for d in range(2):
                for q in range(4):
                    self.stage[slot, 0, d, q] = self.own(m, lax.rem(p + 2, 4), q, d)
                self.far1(m, d).start()

        def S_own(self, m):
            slot, p = lax.rem(m, 2), self.at(m)[0]
            for d in range(2):
                for q in range(4):
                    self.stage[slot, 1, d, q] = self.own(m, step_of(p, d), q, 1 - d)
                self.own1(m, d).start()

        def A1(self, m):
            p = self.at(m)[0]
            arrived(m, self.base, self.bx.at[m, 0])
            for d in range(2):
                for q in range(4):
                    self.bx[m, 0, d, q] += self.own(m, step_of(p, d), q, d)
                self.acc1(m, d).start()

        def F1(self, m):
            p = self.at(m)[0]
            arrived(m, self.base + 1, self.bx.at[m, pl.ds(1, 2)])
            for h in range(2):
                for q in range(4):
                    self.bx[m, 2, h, q] += self.own(m, p, q, h) + self.bx[m, 1, 1 - h, q]
            for d in range(2):
                self.far2(m, d).start()
            for d in range(2):
                self.own2(m, d).start()

        def A2(self, m):
            q = self.at(m)[1]
            arrived(m, self.base + 2, self.by.at[m, 0])
            for d in range(2):
                self.by[m, 0, d] += self.bx[m, 2, d, step_of(q, d)]
                self.acc2(m, d).start()

        def F2(self, m):
            q = self.at(m)[1]
            arrived(m, self.base + 3, self.by.at[m, pl.ds(1, 2)])
            for h in range(2):
                self.by[m, 2, h] += self.bx[m, 2, h, q] + self.by[m, 1, 1 - h]
            self.last(m).start()

        def arrive(self, m):
            self.last(m).wait_recv()

        def total(self, m, rows):
            return self.by[m, 2, z, rows] + self.bz[m, rows]

        def staged(self, m):
            left(m, self.stage.at[lax.rem(m, 2)], self.kind)

    class ZFirst:
        def us(self, m, j):
            return lax.rem(place(m)[0] + (2, 1, 3, 0)[j], 4)

        def zsend(self, m, j):
            return remote(m, 10 + j // 2, S2.at[lax.rem(m, 2), self.us(m, j)], Z2.at[m, self.us(m, j)],
                          to(m, "z", 0), 2)

        def far1(self, m, d):
            return remote(m, 12, Z2.at[m, self.us(m, 0), pl.ds(2 * d, 2)],
                          X2.at[m, 0, pl.ds(2 * d, 2)], to(m, "u", d))

        def own1(self, m, d):
            return remote(m, 13, Z2.at[m, self.us(m, 1 + d), pl.ds(2 - 2 * d, 2)],
                          X2.at[m, 1, pl.ds(2 - 2 * d, 2)], to(m, "u", d))

        def acc1(self, m, d):
            return remote(m, 13, X2.at[m, 0, pl.ds(2 * d, 2)], X2.at[m, 2, pl.ds(2 * d, 2)],
                          to(m, "u", d))

        def far2(self, m, d):
            part = pl.ds(*PARTS[d])
            return remote(m, 14, X2.at[m, 2, lax.rem(place(m)[1] + 2, 4), part],
                          Y2.at[m, 0, part], to(m, "v", d))

        def own2(self, m, d):
            part = pl.ds(*PARTS[1 - d])
            return remote(m, 15, X2.at[m, 2, step_of(place(m)[1], d), part],
                          Y2.at[m, 1, part], to(m, "v", d))

        def acc2(self, m, d):
            part = pl.ds(*PARTS[d])
            return remote(m, 15, Y2.at[m, 0, part], Y2.at[m, 2, part], to(m, "v", d))

        def S(self, m, js):
            slot = lax.rem(m, 2)
            for j in js:
                for v in range(4):
                    S2[slot, self.us(m, j), v] = local(2, m, self.us(m, j), v, 1 - z)
                self.zsend(m, j).start()

        def Z(self, m, j):
            for v in range(4):
                Z2[m, self.us(m, j), v] += local(2, m, self.us(m, j), v, z)

        def Z1a(self, m):
            arrived(m, 10, Z2.at[m, pl.ds(0, 2)])
            self.Z(m, 0)
            for d in range(2):
                self.far1(m, d).start()
            self.Z(m, 1)
            self.own1(m, 0).start()

        def Z1b(self, m):
            arrived(m, 11, Z2.at[m, pl.ds(0, 2)])
            self.Z(m, 2)
            self.own1(m, 1).start()
            self.Z(m, 3)

        def A1(self, m):
            arrived(m, 12, X2.at[m, 0])
            for d in range(2):
                for i in range(2):
                    X2[m, 0, 2 * d + i] += Z2[m, self.us(m, 1 + d), 2 * d + i]
                self.acc1(m, d).start()

        def F1(self, m):
            arrived(m, 13, X2.at[m, pl.ds(1, 2)])
            for v in range(4):
                X2[m, 2, v] += Z2[m, place(m)[0], v] + X2[m, 1, v]
            for d in range(2):
                self.far2(m, d).start()
            for d in range(2):
                self.own2(m, d).start()

        def A2(self, m):
            arrived(m, 14, Y2.at[m, 0])
            for d in range(2):
                part = pl.ds(*PARTS[d])
                Y2[m, 0, part] += X2[m, 2, step_of(place(m)[1], d), part]
                self.acc2(m, d).start()

        def arrive(self, m):
            arrived(m, 15, Y2.at[m, pl.ds(1, 2)])

        def total(self, m, rows):
            return X2[m, 2, place(m)[1], rows] + Y2[m, 1, rows] + Y2[m, 2, rows]

        def staged(self, m):
            left(m, S2.at[lax.rem(m, 2)], 2)

    A = Plane(0, "u", "v", S0, X0, Y0, Z0)
    B = Plane(1, "v", "u", S1b, X1, Y1, Z1)
    C = ZFirst()

    def begin(m):
        @pl.when(m >= 2)
        def _():
            for color in (A, B, C):
                color.staged(m - 2)

        load_g(m, 0).wait()
        B.S_far(m)
        load_g(m, 1).wait()
        A.S_far(m)
        load_g(m, 2).wait()
        C.S(m, (0,))

        @pl.when(m + 2 < N)
        def _():
            for i in range(3):
                load_g(m + 2, i).start()

        B.S_own(m)
        A.S_own(m)
        C.S(m, (1, 2, 3))
        for c in load_state(m):
            c.wait()

        @pl.when(m == 0)
        def _():
            for c in scalars:
                c.wait()

        @pl.when(m + 1 < N)
        def _():
            for c in load_state(m + 1):
                c.start()

    def update(m, color, r0, size):
        color.arrive(m)
        t, g = lax.div(m, 2), lax.rem(m, 2)
        scale, top = ms_ref[t], vm_ref[g, t]
        inverse = 1.0 / jnp.full((8, LANES), ve_ref[g, t], jnp.float32)[0:1]
        hi = peak = jnp.zeros((8, LANES), jnp.float32)
        lo = hi + 3e38
        at = r0
        while at < r0 + size:
            base = at // 16 * 16
            rows = min(base + 32 if base == at else base + 16, r0 + size) - at
            here = pl.ds(at, rows)
            half = lambda ref: ref[m, base : base + 32 if rows > 16 else base + 16].astype(
                jnp.float32
            )[at - base : at - base + rows]
            gr = color.total(m, pl.ds(at - r0, rows)) * (1.0 / 32)
            m_old = scale * half(qm)
            v_old = top * jnp.exp(jnp.log(half(qv)) * inverse)
            m_new = 0.9 * m_old + 0.1 * gr
            v_new = 0.95 * v_old + 0.05 * gr * gr
            w = par[m, here]
            par[m, here] = w - 0.02 * (m_new / (jnp.sqrt(v_new) + 1e-8) + 0.1 * w)
            mnew[m, here] = m_new
            lv[m, here] = jnp.log(v_new)
            fold = lambda v: v.reshape(rows // 8, 8, LANES)
            hi = jnp.maximum(hi, jnp.max(fold(v_new), axis=0))
            lo = jnp.minimum(lo, jnp.min(fold(v_new), axis=0))
            peak = jnp.maximum(peak, jnp.max(fold(jnp.abs(m_new)), axis=0))
            at += rows
        for i, v in enumerate((hi, -lo, peak)):
            most[i, m] = jnp.maximum(most[i, m], v)

    def drain(m):
        left(m, G.at[m, :, :, :, pl.ds(0, 240)])

    def update_c(m):
        pl.when(m >= 1)(lambda: drain(m - 1))
        update(m, C, 168, 88)

    most[...] = jnp.full(most.shape, -3e38, jnp.float32)
    ops = dict(S1=begin, A1y=B.A1, A1x=A.A1, Z1a=C.Z1a, Z1b=C.Z1b, F1y=B.F1, F1x=A.F1,
               A2z=C.A1, A2y=B.A2, A2x=A.A2, F2z=C.F1, F2y=B.F2, F2x=A.F2, A3z=C.A2,
               EA=lambda m: update(m, A, 0, 64), EB=lambda m: update(m, B, 64, 104), EC=update_c)
    assert all(LAGS["EC"] + 1 > v for v in LAGS.values())

    flip = lambda v, b: v + b - 2 * b * v
    plane_peers = [
        {"y": lax.rem(y + j, 4), "x": lax.rem(x + k, 4)}
        for j in (2, 1, 3, 0) for k in (2, 1, 3, 0) if j or k
    ]
    column_peers = [
        {"zl": flip(z, i & 1), "core": flip(core, i >> 1 & 1), "zh": flip(zh, i >> 2)}
        for i in range(7, 0, -1)
    ]

    for i in range(3):
        load_g(0, i).start()
    barrier = pltpu.get_barrier_semaphore()
    peers = [to(0, axis, d) for axis in ("u", "v") for d in range(2)]
    peers += [p for i, p in enumerate(column_peers) if i not in (1, 3)]
    for peer in peers:
        pl.semaphore_signal(barrier, inc=1, device_id=peer, device_id_type=MESH)
    pl.semaphore_wait(barrier, len(peers))
    for i in range(3):
        load_g(1, i).start()
    for c in load_state(0) + scalars:
        c.start()

    def step(k, _):
        for name in ORDER:
            m = k - LAGS[name]
            pl.when((m >= 0) & (m < N))(lambda f=ops[name], m=m: f(m))
        return 0

    lax.fori_loop(0, N + max(LAGS.values()), step, 0)

    sub = lax.broadcasted_iota(jnp.int32, (N, LANES), 0)
    lane = lax.broadcasted_iota(jnp.int32, (N, LANES), 1)
    spread = jnp.full((N, LANES), -3e38, jnp.float32)
    for i in range(3):
        v = jnp.max(jnp.max(most[i], axis=1), axis=1, keepdims=True)
        spread = jnp.where(lane == 8 * i + 4 * lax.rem(sub, 2) + lax.div(sub, 2), v, spread)
    stat[0:1] = jnp.max(spread, axis=0, keepdims=True)
    lane = lane[0:1]
    for phase, (who, buf) in enumerate(((plane_peers, wide), (column_peers, deep))):
        copies = [
            pltpu.make_async_remote_copy(
                src_ref=stat.at[pl.ds(8 * phase, 1)], dst_ref=buf.at[pl.ds(i, 1)],
                send_sem=atsem.at[phase], recv_sem=asem.at[phase],
                device_id=peer, device_id_type=MESH,
            )
            for i, peer in enumerate(who)
        ]
        for c in copies:
            c.start()
        mine = stat[8 * phase : 8 * phase + 1]
        buf[len(who) : len(who) + 1] = mine
        if phase == 0:
            drain(N - 1)
            for m in (N - 2, N - 1):
                for color in (A, B, C):
                    color.staged(m)
        everyone = pltpu.make_async_remote_copy(
            src_ref=buf.at[pl.ds(0, len(who))], dst_ref=buf.at[pl.ds(0, len(who))],
            send_sem=atsem.at[phase], recv_sem=asem.at[phase],
            device_id=who[0], device_id_type=MESH,
        )
        everyone.wait_recv()
        top = jnp.max(buf[0 : len(who) + 1], axis=0, keepdims=True)
        if phase == 0:
            stat[8:9] = top
        else:
            table[...] = jnp.where(lane < 16, jnp.maximum(mine, buf[6:7]), top)
        everyone.wait_send()


def finish(par, mnew, lv, table, np_hbm, nqm_hbm, nms_ref, nqv_hbm, nvm_ref, nve_ref, qmo, qvo, sem):
    def store_out(m, i):
        h, v = ((np_hbm, par), (nqm_hbm, qmo), (nqv_hbm, qvo))[i]
        return pltpu.make_async_copy(v.at[m], columns(h, m), sem.at[i])

    for m in range(N):
        store_out(m, 0).start()
    row = table[...]
    lane = lax.broadcasted_iota(jnp.int32, (1, LANES), 1)
    left = lambda v, k: pltpu.roll(v, LANES - k, 1)
    low, peak = -left(row, 8), left(row, 16)
    scale = jnp.maximum(peak, left(peak, 4)) + 1e-6
    new_exp = 12.343 / jnp.maximum(jnp.log(row / low), 1.0)
    log_top, inverse = jnp.log(row), 1.0 / scale
    pick = lambda v, i: jnp.max(jnp.where(lane == i, v, -3e38), axis=1, keepdims=True)
    for m in range(N):
        t, g = m // 2, m % 2
        qmo[m] = (mnew[m] * pick(inverse, t)).astype(jnp.bfloat16)
        store_out(m, 1).start()
        e, top = pick(new_exp, 4 * g + t), pick(log_top, 4 * g + t)
        qvo[m] = jnp.exp(e * (lv[m] - top)).astype(jnp.bfloat16)
        store_out(m, 2).start()
    nms_ref[...] = scale[:, 0:4]
    for g in range(2):
        nvm_ref[g : g + 1, :] = left(row, 4 * g)[:, 0:4] if g else row[:, 0:4]
        nve_ref[g : g + 1, :] = left(new_exp, 4 * g)[:, 0:4] if g else new_exp[:, 0:4]
    for i, h in enumerate((np_hbm, nqm_hbm, nqv_hbm)):
        pltpu.make_async_copy(h, h, sem.at[i]).wait()


def on_device(grads, param, q_m, m_scale, q_v, v_max, v_exp):
    f32, bf16 = jnp.float32, jnp.bfloat16
    a, b, c = SPLIT
    plane = lambda s: [
        pltpu.VMEM((2, 2, 2, 4, s, LANES), f32),
        pltpu.VMEM((N, 3, 2, 4, s, LANES), f32),
        pltpu.VMEM((N, 3, 2, s, LANES), f32),
        pltpu.VMEM((N, s, LANES), f32),
    ]
    block = lambda kind: pltpu.VMEM((N, ROWS, LANES), kind)
    anywhere = pl.BlockSpec(memory_space=pl.ANY)
    vmem = pl.BlockSpec(memory_space=pltpu.VMEM)
    kept = pl.pallas_call(
        kernel,
        out_shape=(block(f32), block(f32), block(f32), pltpu.VMEM((1, LANES), f32)),
        in_specs=[anywhere] * 7,
        out_specs=(vmem,) * 4,
        scratch_shapes=[
            pltpu.VMEM((N, 4, 4, 2, ROWS, LANES), bf16),
            *plane(a),
            *plane(b),
            pltpu.VMEM((2, 4, 4, c, LANES), f32),
            pltpu.VMEM((N, 4, 4, c, LANES), f32),
            pltpu.VMEM((N, 3, 4, c, LANES), f32),
            pltpu.VMEM((N, 3, c, LANES), f32),
            block(bf16), block(bf16),
            pltpu.VMEM((3, N, 8, LANES), f32),
            pltpu.VMEM((24, LANES), f32),
            pltpu.VMEM((32, LANES), f32),
            pltpu.VMEM((16, LANES), f32),
            pltpu.SMEM((4,), f32),
            pltpu.SMEM((2, 4), f32),
            pltpu.SMEM((2, 4), f32),
            pltpu.SemaphoreType.DMA((N, SEMS)),
            pltpu.SemaphoreType.DMA((N,)),
            pltpu.SemaphoreType.DMA((2, 3)),
            pltpu.SemaphoreType.DMA((2, 3)),
            pltpu.SemaphoreType.DMA((3,)),
            pltpu.SemaphoreType.DMA((2,)),
            pltpu.SemaphoreType.DMA((2,)),
            pltpu.SemaphoreType.DMA((3,)),
        ],
        compiler_params=pltpu.CompilerParams(
            collective_id=0, has_side_effects=True, vmem_limit_bytes=LIMIT
        ),
    )(grads[0].reshape(4, 4, 4, 2, ROWS, 2 * LANES), param, q_m, m_scale, q_v, v_max.T, v_exp.T)
    small = lambda rows: jax.ShapeDtypeStruct((rows, 4), f32)
    new_param, new_q_m, ms, new_q_v, vm, ve = pl.pallas_call(
        finish,
        out_shape=(
            jax.ShapeDtypeStruct(param.shape, f32),
            jax.ShapeDtypeStruct(q_m.shape, bf16),
            small(1),
            jax.ShapeDtypeStruct(q_v.shape, bf16),
            small(2),
            small(2),
        ),
        in_specs=[vmem] * 4,
        out_specs=(anywhere, anywhere, vmem, anywhere, vmem, vmem),
        scratch_shapes=[block(bf16), block(bf16), pltpu.SemaphoreType.DMA((3,))],
        compiler_params=pltpu.CompilerParams(vmem_limit_bytes=8 * 2**20),
    )(*kept)
    return new_param, new_q_m, ms[0], new_q_v, vm.T, ve.T


def solution(mesh):
    split = Mesh(mesh.devices.reshape(2, 2, 4, 4, 2), TENSOR + DP)
    return jax.shard_map(
        on_device,
        mesh=split,
        in_specs=(
            P(DP, None, None, TENSOR),
            P(None, DP, TENSOR),
            P(None, DP, TENSOR),
            P(),
            P(None, DP, TENSOR),
            P(None, TENSOR),
            P(None, TENSOR),
        ),
        out_specs=(
            P(None, DP, TENSOR),
            P(None, DP, TENSOR),
            P(),
            P(None, DP, TENSOR),
            P(None, TENSOR),
            P(None, TENSOR),
        ),
        check_vma=False,
    )
```
